64 devices in a mesh: data: 4 (over x, y), seq: 16 (over z, core).
Axes of the slice: x: 2, y: 2, z: 8, core: 2. Of those that a mesh axis runs over, the one named last changes fastest.
The devices are a block of a 4x4x8 slice.
Arguments:
- x_in: bfloat16 [16384, 2560], P(('data', 'seq')), parts along dimension 0
- g_attn: float32 [2560], replicated
- w_qkv: bfloat16 [2560, 7680], replicated
- w_out: bfloat16 [32, 80, 2560], replicated
- g_mlp: float32 [2560], replicated
- w_gate: bfloat16 [2560, 10240], replicated
- w_up: bfloat16 [2560, 10240], replicated
- w_down: bfloat16 [10240, 2560], replicated
Outputs:
- output: bfloat16 [16384, 2560], P(('data', 'seq')), parts along dimension 0
There are 4 independent parts. The reference program is written for one: setup_inputs(seed, part) draws one part's arguments, and reference() takes and returns one part's arrays. A program takes and returns all parts, laid end to end along the dimension named above; an argument that names none is the same for every part.
All inputs are finite; a program needn't handle non-finite values.
Results may differ from the reference program's by a relative error of at most 0.00722409.
Values are sent between devices in bfloat16 or wider.
A program may use at most 768 MiB of HBM per device.

```python
import jax
import jax.numpy as jnp
from jax import lax

SEQ_LEN = 4096
BLOCK_ROWS = 256
D = 2560
HEADS = 32
HEAD = 80
FF = 10240
ROPE_BASE = 10000
WALK_RANK = 8


def setup_inputs(seed: int = 0, part: int = 0) -> dict:
    part_key = jax.random.fold_in(jax.random.key(seed), part)
    noise_key, walk_key, mix_key = jax.random.split(part_key, 3)
    weight_keys = jax.random.split(jax.random.key(seed + 1), 7)
    inner_width = HEADS * HEAD
    walk_path = jnp.cumsum(jax.random.normal(walk_key, (SEQ_LEN, WALK_RANK), jnp.float32), axis=0)
    walk_path = walk_path - jnp.mean(walk_path, axis=0, keepdims=True)
    walk_path = walk_path / jnp.sqrt(jnp.mean(walk_path * walk_path) + 1e-6)
    mixing = jax.random.normal(mix_key, (WALK_RANK, D), jnp.float32) * WALK_RANK ** -0.5
    x_val = 0.5 * jax.random.normal(noise_key, (SEQ_LEN, D), jnp.float32) + jnp.dot(walk_path, mixing)
    return {
        'x_in': x_val.astype(jnp.bfloat16),
        'g_attn': jax.random.uniform(weight_keys[0], (D,), jnp.float32, 0.5, 1.5),
        'w_qkv': (jax.random.normal(weight_keys[1], (D, 3 * inner_width), jnp.float32) * D ** -0.5).astype(jnp.bfloat16),
        'w_out': (jax.random.normal(weight_keys[2], (HEADS, HEAD, D), jnp.float32) * 1.5 * inner_width ** -0.5).astype(jnp.bfloat16),
        'g_mlp': jax.random.uniform(weight_keys[3], (D,), jnp.float32, 0.5, 1.5),
        'w_gate': (jax.random.normal(weight_keys[4], (D, FF), jnp.float32) * D ** -0.5).astype(jnp.bfloat16),
        'w_up': (jax.random.normal(weight_keys[5], (D, FF), jnp.float32) * D ** -0.5).astype(jnp.bfloat16),
        'w_down': (jax.random.normal(weight_keys[6], (FF, D), jnp.float32) * FF ** -0.5).astype(jnp.bfloat16),
    }


def rms_norm(row_vals, gain_vec):
    rows_f32 = row_vals.astype(jnp.float32)
    inv_rms = lax.rsqrt(jnp.mean(rows_f32 * rows_f32, axis=-1, keepdims=True) + 1e-5)
    return (rows_f32 * inv_rms * gain_vec).astype(jnp.bfloat16)


def rope_tables(positions):
    inv_freq = 1.0 / (ROPE_BASE ** (jnp.arange(0, HEAD, 2, dtype=jnp.float32) / HEAD))
    angles = positions.astype(jnp.float32)[:, None] * inv_freq[None, :]
    angles = jnp.concatenate([angles, angles], axis=-1)
    return jnp.cos(angles), jnp.sin(angles)


def apply_rope(qk_pair, cos_tab, sin_tab):
    half_dim = qk_pair.shape[-1] // 2
    rotated = jnp.concatenate([-qk_pair[..., half_dim:], qk_pair[..., :half_dim]], axis=-1)
    return qk_pair * cos_tab + rotated * sin_tab


def reference(x_in, g_attn, w_qkv, w_out, g_mlp, w_gate, w_up, w_down):
    inner_width = HEADS * HEAD
    x_norm = rms_norm(x_in, g_attn)
    qkv_f32 = jnp.dot(x_norm, w_qkv, preferred_element_type=jnp.float32).reshape(SEQ_LEN, 3, HEADS, HEAD)
    cos_tab, sin_tab = rope_tables(jnp.arange(SEQ_LEN))
    qk_rot = apply_rope(qkv_f32[:, :2], cos_tab[:, None, None, :], sin_tab[:, None, None, :])
    query_f32 = qk_rot[:, 0].astype(jnp.bfloat16).astype(jnp.float32)
    key_f32 = qk_rot[:, 1].astype(jnp.bfloat16).astype(jnp.float32)
    value_f32 = qkv_f32[:, 2].astype(jnp.bfloat16).astype(jnp.float32)
    score_scale = HEAD ** -0.5
    key_pos = jnp.arange(SEQ_LEN)

    def one_block(block_idx):
        row_start = block_idx * BLOCK_ROWS
        q_blk = lax.dynamic_slice_in_dim(query_f32, row_start, BLOCK_ROWS, axis=0)
        scores = jnp.einsum('qhd,khd->hqk', q_blk, key_f32) * score_scale
        query_pos = row_start + jnp.arange(BLOCK_ROWS)
        allowed = key_pos[None, :] <= query_pos[:, None]
        scores = jnp.where(allowed[None], scores, -jnp.inf)
        attn_probs = jax.nn.softmax(scores, axis=-1).astype(jnp.bfloat16).astype(jnp.float32)
        return jnp.einsum('hqk,khd->qhd', attn_probs, value_f32).astype(jnp.bfloat16)

    attn_rows = lax.map(one_block, jnp.arange(SEQ_LEN // BLOCK_ROWS)).reshape(SEQ_LEN, inner_width)
    attn_mixed = jnp.dot(attn_rows, w_out.reshape(inner_width, D), preferred_element_type=jnp.float32)
    y_rows = (x_in.astype(jnp.float32) + attn_mixed).astype(jnp.bfloat16)
    y_norm = rms_norm(y_rows, g_mlp)
    gate_pre = jnp.dot(y_norm, w_gate, preferred_element_type=jnp.float32)
    up_pre = jnp.dot(y_norm, w_up, preferred_element_type=jnp.float32)
    hidden = (jax.nn.silu(gate_pre) * up_pre).astype(jnp.bfloat16)
    return (y_rows.astype(jnp.float32) + jnp.dot(hidden, w_down, preferred_element_type=jnp.float32)).astype(jnp.bfloat16)
```

```python
import functools
import math

import jax
import jax.numpy as jnp
from jax import lax
from jax.experimental import pallas as pl
from jax.experimental.pallas import tpu as pltpu
from jax.sharding import PartitionSpec as P

ROPE_BASE = 10000
LOG2E = math.log2(math.e)


def rms_norm(row_vals, gain_vec):
    rows_f32 = row_vals.astype(jnp.float32)
    inv_rms = lax.rsqrt(jnp.mean(rows_f32 * rows_f32, axis=-1, keepdims=True) + 1e-5)
    return (rows_f32 * inv_rms * gain_vec).astype(jnp.bfloat16)


def rope_tables_t(positions, head_dim):
    inv_freq = 1.0 / (ROPE_BASE ** (jnp.arange(0, head_dim, 2, dtype=jnp.float32) / head_dim))
    angles = inv_freq[:, None] * positions.astype(jnp.float32)[None, :]
    return jnp.cos(angles), jnp.sin(angles)


def attention_kernel(n, hpd, hd, group, x_ref, g_ref, cos_ref, sin_ref, w_ref, o_ref,
                     wbuf, xn, sendb, recvb, kbuf, osend, orecv, wsem, ssem, rsem, osem, orsem):
    rows = x_ref.shape[0]
    inner = n * hpd * hd
    gcols = group * hpd * hd
    ngroups = n // group
    me = lax.axis_index('seq')
    mygrp = me // group

    def w_copy(g, t):
        grp = lax.rem(mygrp + ngroups // 2 + g, ngroups)
        col = pl.multiple_of(t * inner + grp * gcols, 128)
        return pltpu.make_async_copy(w_ref.at[:, pl.ds(col, gcols)], wbuf.at[t], wsem.at[t])

    for t in range(3):
        w_copy(0, t).start()

    barrier = pltpu.get_barrier_semaphore()

    def greet(k, c):
        pl.semaphore_signal(barrier, inc=1, device_id={'seq': lax.rem(me + k, n)}, device_id_type=pl.DeviceIdType.MESH)
        return c

    lax.fori_loop(1, n, greet, 0)
    xn[...] = rms_norm(x_ref[...], g_ref[...])
    pl.semaphore_wait(barrier, n - 1)

    def qkv_send(dest, h):
        return pltpu.make_async_remote_copy(
            src_ref=sendb.at[dest, h], dst_ref=recvb.at[me, h], send_sem=ssem.at[dest, h], recv_sem=rsem.at[me, h],
            device_id={'seq': dest}, device_id_type=pl.DeviceIdType.MESH)

    def qkv_recv(src, h):
        return pltpu.make_async_remote_copy(
            src_ref=sendb.at[src, h], dst_ref=recvb.at[src, h], send_sem=ssem.at[src, h], recv_sem=rsem.at[src, h],
            device_id={'seq': src}, device_id_type=pl.DeviceIdType.MESH)

    def qkv_local(h):
        return pltpu.make_async_copy(sendb.at[me, h], recvb.at[me, h], rsem.at[me, h])

    def project(g, c):
        grp = lax.rem(mygrp + ngroups // 2 + g, ngroups)
        for t in range(3):
            w_copy(g, t).wait()
            acc = jnp.dot(xn[...], wbuf[t], preferred_element_type=jnp.float32)

            @pl.when(g < ngroups - 1)
            def _():
                w_copy(g + 1, t).start()

            acc_t = acc.T
            for k in range(group * hpd):
                u = acc_t[k * hd:(k + 1) * hd]
                if t < 2:
                    lo, hi = u[:hd // 2], u[hd // 2:]
                    cos, sin = cos_ref[...], sin_ref[...]
                    u = jnp.concatenate([lo * cos - hi * sin, hi * cos + lo * sin], axis=0)
                sendb[grp * group + k // hpd, k % hpd, t * hd:(t + 1) * hd, :] = u.astype(jnp.bfloat16)

        def first_head(k, c):
            dest = grp * group + k

            @pl.when(dest != me)
            def _():
                qkv_send(dest, 0).start()
            return c

        lax.fori_loop(0, group, first_head, 0)
        return c

    lax.fori_loop(0, ngroups, project, 0)

    for h in range(hpd):
        qkv_local(h).start()

        if h > 0:
            def later_head(k, c):
                qkv_send(lax.rem(me + k, n), h).start()
                return c

            lax.fori_loop(1, n, later_head, 0)

    def o_send(dest, h):
        return pltpu.make_async_remote_copy(
            src_ref=osend.at[dest, h], dst_ref=orecv.at[me, h], send_sem=osem.at[dest, h], recv_sem=orsem.at[me, h],
            device_id={'seq': dest}, device_id_type=pl.DeviceIdType.MESH)

    def o_recv(src, h):
        return pltpu.make_async_remote_copy(
            src_ref=osend.at[src, h], dst_ref=orecv.at[src, h], send_sem=osem.at[src, h], recv_sem=orsem.at[src, h],
            device_id={'seq': src}, device_id_type=pl.DeviceIdType.MESH)

    def o_local(h):
        return pltpu.make_async_copy(osend.at[me, h], orecv.at[me, h], orsem.at[me, h])

    per = 2
    tile = per * rows
    scale2 = LOG2E * hd ** -0.5

    for h in range(hpd):
        def arrive(src, c):
            @pl.when(src != me)
            def _():
                qkv_recv(src, h).wait_recv()

            @pl.when(src == me)
            def _():
                qkv_local(h).wait()

            kbuf[pl.ds(pl.multiple_of(src * rows, rows), rows), :] = recvb[src, h, hd:2 * hd, :].T
            return c

        lax.fori_loop(0, n, arrive, 0)

        def q_tile(i, c):
            q_t = jnp.concatenate([recvb[per * i + r, h, 0:hd, :] for r in range(per)], axis=1)

            def scores(j):
                k_blk = kbuf[pl.ds(pl.multiple_of(j * tile, tile), tile), :]
                return jnp.dot(k_blk, q_t, preferred_element_type=jnp.float32)

            def values(j):
                return jnp.concatenate([recvb[per * j + r, h, 2 * hd:3 * hd, :] for r in range(per)], axis=1)

            s = scores(i)
            key_pos = lax.broadcasted_iota(jnp.int32, s.shape, 0)
            query_pos = lax.broadcasted_iota(jnp.int32, s.shape, 1)
            s = jnp.where(key_pos <= query_pos, s, -jnp.inf)
            m = jnp.max(s, axis=0, keepdims=True)
            p = jnp.exp2((s - m) * scale2)
            l = jnp.sum(p, axis=0, keepdims=True)
            acc = jnp.dot(values(i), p.astype(jnp.bfloat16), preferred_element_type=jnp.float32)

            def kv_tile(j, carry):
                m, l, acc = carry
                s = scores(j)
                m_new = jnp.maximum(m, jnp.max(s, axis=0, keepdims=True))
                p = jnp.exp2((s - m_new) * scale2)
                alpha = jnp.exp2((m - m_new) * scale2)
                l = alpha * l + jnp.sum(p, axis=0, keepdims=True)
                acc = alpha * acc + jnp.dot(values(j), p.astype(jnp.bfloat16), preferred_element_type=jnp.float32)
                return m_new, l, acc

            m, l, acc = lax.fori_loop(0, i, kv_tile, (m, l, acc))
            out = (acc / l).astype(jnp.bfloat16)
            for r in range(per):
                dest = per * i + r
                osend[dest, h] = out[:, r * rows:(r + 1) * rows]

                @pl.when(dest != me)
                def _():
                    o_send(dest, h).start()

                @pl.when(dest == me)
                def _():
                    o_local(h).start()
            return c

        lax.fori_loop(0, n // per, q_tile, 0)

    def finish(k, c):
        other = lax.rem(me + k, n)
        for h in range(hpd):
            o_recv(other, h).wait_recv()
            qkv_send(other, h).wait_send()
            o_send(other, h).wait_send()
        return c

    lax.fori_loop(1, n, finish, 0)
    for h in range(hpd):
        o_local(h).wait()
    o_ref[...] = orecv[...]


def attention_rows(x_blk, g_attn, w_qkv, cos_t, sin_t, n, n_heads, head_dim):
    rows, width = x_blk.shape
    hpd = n_heads // n
    group = 1
    while (group * hpd * head_dim) % 128:
        group *= 2
    gcols = group * hpd * head_dim
    vmem = pl.BlockSpec(memory_space=pltpu.VMEM)
    kernel = functools.partial(attention_kernel, n, hpd, head_dim, group)
    bf16 = jnp.bfloat16
    return pl.pallas_call(
        kernel,
        out_shape=jax.ShapeDtypeStruct((n, hpd, head_dim, rows), bf16),
        in_specs=[vmem, vmem, vmem, vmem, pl.BlockSpec(memory_space=pl.ANY)],
        out_specs=vmem,
        scratch_shapes=[
            pltpu.VMEM((3, width, gcols), bf16),
            pltpu.VMEM((rows, width), bf16),
            pltpu.VMEM((n, hpd, 3 * head_dim, rows), bf16),
            pltpu.VMEM((n, hpd, 3 * head_dim, rows), bf16),
            pltpu.VMEM((n * rows, head_dim), bf16),
            pltpu.VMEM((n, hpd, head_dim, rows), bf16),
            pltpu.VMEM((n, hpd, head_dim, rows), bf16),
            pltpu.SemaphoreType.DMA((3,)),
            pltpu.SemaphoreType.DMA((n, hpd)),
            pltpu.SemaphoreType.DMA((n, hpd)),
            pltpu.SemaphoreType.DMA((n, hpd)),
            pltpu.SemaphoreType.DMA((n, hpd)),
        ],
        compiler_params=pltpu.CompilerParams(collective_id=0, has_side_effects=True, vmem_limit_bytes=60 * 1024 * 1024),
        name='attention',
    )(x_blk, g_attn, cos_t, sin_t, w_qkv)


def gated_mlp(y_rows, g_mlp, w_gate, w_up, w_down):
    y_norm = rms_norm(y_rows, g_mlp)
    gate_pre = jnp.dot(y_norm, w_gate, preferred_element_type=jnp.float32)
    up_pre = jnp.dot(y_norm, w_up, preferred_element_type=jnp.float32)
    hidden = (jax.nn.silu(gate_pre) * up_pre).astype(jnp.bfloat16)
    return (y_rows.astype(jnp.float32) + jnp.dot(hidden, w_down, preferred_element_type=jnp.float32)).astype(jnp.bfloat16)


def solution(mesh):
    n = mesh.shape['seq']

    def local_layer(x_blk, g_attn, w_qkv, w_out, g_mlp, w_gate, w_up, w_down):
        n_heads, head_dim, model_width = w_out.shape
        local_rows = x_blk.shape[0]
        member = lax.axis_index('seq')
        positions = member * local_rows + jnp.arange(local_rows)
        cos_t, sin_t = rope_tables_t(positions, head_dim)
        o_t = attention_rows(x_blk, g_attn[None, :], w_qkv, cos_t, sin_t, n, n_heads, head_dim)
        o_t = o_t.reshape(n_heads * head_dim, local_rows)
        attn_mixed = lax.dot_general(o_t, w_out.reshape(n_heads * head_dim, model_width), (((0,), (0,)), ((), ())),
                                     preferred_element_type=jnp.float32)
        y_rows = (x_blk.astype(jnp.float32) + attn_mixed).astype(jnp.bfloat16)
        return gated_mlp(y_rows, g_mlp, w_gate, w_up, w_down)

    row_spec = P(('data', 'seq'), None)
    return jax.shard_map(local_layer, mesh=mesh, in_specs=(row_spec, P(), P(), P(), P(), P(), P(), P()), out_specs=row_spec, check_vma=False)
```

```python
import functools
import math

import jax
import jax.numpy as jnp
from jax import lax
from jax.experimental import pallas as pl
from jax.experimental.pallas import tpu as pltpu
from jax.sharding import PartitionSpec as P

ROPE_BASE = 10000
LOG2E = math.log2(math.e)
HALVES = 2
MESH = pl.DeviceIdType.MESH


def rms_norm(row_vals, gain_vec):
    rows_f32 = row_vals.astype(jnp.float32)
    inv_rms = lax.rsqrt(jnp.mean(rows_f32 * rows_f32, axis=-1, keepdims=True) + 1e-5)
    return (rows_f32 * inv_rms * gain_vec).astype(jnp.bfloat16)


def rope_tables_t(positions, head_dim):
    inv_freq = 1.0 / (ROPE_BASE ** (jnp.arange(0, head_dim, 2, dtype=jnp.float32) / head_dim))
    angles = inv_freq[:, None] * positions.astype(jnp.float32)[None, :]
    return jnp.cos(angles), jnp.sin(angles)


def layer_kernel(n, hpd, hd, group, chunk, slots,
                 x_ref, ga_ref, gm_ref, cos_ref, sin_ref, wqkv_ref, wout_ref, wg_ref, wu_ref, wd_ref, z_ref,
                 wout, xn, kvs, kvr, qs, qr, kbuf, osend, orecv, yn, ybuf, acc, zrecv, wg, wu, wd,
                 stage_sem, wout_sem, w_sem, kv_ss, kv_rs, q_ss, q_rs, o_ss, o_rs, y_ss, y_rs, z_ss, z_rs):
    rows, width = x_ref.shape
    half_rows = rows // HALVES
    inner = n * hpd * hd
    gcols = group * hpd * hd
    ngroups = n // group
    stages = width // gcols
    ff_half = wg_ref.shape[1] // 2
    nchunks = ff_half // chunk
    me = lax.axis_index('seq')
    core = lax.rem(me, 2)
    partner = me + 1 - 2 * core
    mygrp = me // group

    def grp_of(g):
        return lax.rem(mygrp + ngroups // 2 + g, ngroups)

    def tile_copy(s, t, g):
        col = pl.multiple_of(t * inner + grp_of(g) * gcols, 128)
        slot = pl.multiple_of(lax.rem(s, stages) * gcols, 128)
        return pltpu.make_async_copy(wqkv_ref.at[:, pl.ds(col, gcols)], wout.at[:, pl.ds(slot, gcols)],
                                     stage_sem.at[lax.rem(s, stages)])

    def start_tile(s):
        @pl.when(s < 2 * ngroups)
        def _():
            tile_copy(s, 1 + lax.rem(s, 2), s // 2).start()

        @pl.when(jnp.logical_and(s >= 2 * ngroups, s < 3 * ngroups))
        def _():
            tile_copy(s, 0, s - 2 * ngroups).start()

    def chunk_copies(s):
        slot = lax.rem(s, slots)
        ff = pl.multiple_of(core * ff_half + lax.rem(s, nchunks) * chunk, 128)
        return (pltpu.make_async_copy(wg_ref.at[:, pl.ds(ff, chunk)], wg.at[slot], w_sem.at[0, slot]),
                pltpu.make_async_copy(wu_ref.at[:, pl.ds(ff, chunk)], wu.at[slot], w_sem.at[1, slot]),
                pltpu.make_async_copy(wd_ref.at[pl.ds(ff, chunk), :], wd.at[slot], w_sem.at[2, slot]))

    for s in range(stages):
        start_tile(s)

    barrier = pltpu.get_barrier_semaphore()

    def greet(k, c):
        pl.semaphore_signal(barrier, inc=1, device_id={'seq': lax.rem(me + k, n)}, device_id_type=MESH)
        return c

    lax.fori_loop(1, n, greet, 0)
    xn[...] = rms_norm(x_ref[...], ga_ref[...])
    pl.semaphore_wait(barrier, n - 1)

    def remote(src, dst, ssem, rsem, dest):
        return pltpu.make_async_remote_copy(src_ref=src, dst_ref=dst, send_sem=ssem, recv_sem=rsem,
                                            device_id={'seq': dest}, device_id_type=MESH)

    def kv_send(dest, h):
        return remote(kvs.at[dest, h], kvr.at[me, h], kv_ss.at[dest, h], kv_rs.at[me, h], dest)

    def kv_recv(src, h):
        return remote(kvs.at[src, h], kvr.at[src, h], kv_ss.at[src, h], kv_rs.at[src, h], src)

    def kv_local(h):
        return pltpu.make_async_copy(kvs.at[me, h], kvr.at[me, h], kv_rs.at[me, h])

    def q_send(dest, u):
        src, dst = (qs.at[dest, 0], qr.at[me, 0]) if u == 0 else (qs.at[dest, 1, u - 1], qr.at[me, 1, u - 1])
        return remote(src, dst, q_ss.at[dest, u], q_rs.at[me, u], dest)

    def q_recv(src, u):
        a, b = (qs.at[src, 0], qr.at[src, 0]) if u == 0 else (qs.at[src, 1, u - 1], qr.at[src, 1, u - 1])
        return remote(a, b, q_ss.at[src, u], q_rs.at[src, u], src)

    def q_local(u):
        src, dst = (qs.at[me, 0], qr.at[me, 0]) if u == 0 else (qs.at[me, 1, u - 1], qr.at[me, 1, u - 1])
        return pltpu.make_async_copy(src, dst, q_rs.at[me, u])

    def o_send(dest, f):
        return remote(osend.at[f, dest], orecv.at[f, me], o_ss.at[f, dest], o_rs.at[f, me], dest)

    def o_recv(src, f):
        return remote(osend.at[f, src], orecv.at[f, src], o_ss.at[f, src], o_rs.at[f, src], src)

    def o_local(f):
        return pltpu.make_async_copy(osend.at[f, me], orecv.at[f, me], o_rs.at[f, me])

    def project(s):
        start = pl.multiple_of(lax.rem(s, stages) * gcols, 128)
        out = jnp.dot(xn[...], wout[:, pl.ds(start, gcols)], preferred_element_type=jnp.float32)
        start_tile(s + stages)
        return out.T

    def rope(u):
        lo, hi = u[:hd // 2], u[hd // 2:]
        cos, sin = cos_ref[...], sin_ref[...]
        return jnp.concatenate([lo * cos - hi * sin, hi * cos + lo * sin], axis=0)

    def send_group(g, make):
        def one(k, c):
            dest = grp_of(g) * group + k

            @pl.when(dest != me)
            def _():
                make(dest).start()
            return c

        lax.fori_loop(0, group, one, 0)

    def project_kv(g, c):
        for t in (0, 1):
            tile_copy(2 * g + t, 1 + t, g).wait()
            out = project(2 * g + t)
            for k in range(group * hpd):
                u = out[k * hd:(k + 1) * hd]
                if t == 0:
                    u = rope(u)
                kvs[grp_of(g) * group + k // hpd, k % hpd, t * hd:(t + 1) * hd, :] = u.astype(jnp.bfloat16)
        send_group(g, lambda dest: kv_send(dest, 0))
        return c

    lax.fori_loop(0, ngroups, project_kv, 0)
    kv_local(0).start()
    kv_local(1).start()

    def project_q(g, c):
        s = 2 * ngroups + g
        tile_copy(s, 0, g).wait()
        out = project(s)
        for k in range(group * hpd):
            u = rope(out[k * hd:(k + 1) * hd]).astype(jnp.bfloat16)
            for f in range(HALVES):
                qs[grp_of(g) * group + k // hpd, k % hpd, f] = u[:, f * half_rows:(f + 1) * half_rows]
        send_group(g, lambda dest: q_send(dest, 0))
        return c

    lax.fori_loop(0, ngroups, project_q, 0)
    for u in range(3):
        q_local(u).start()

    def to_others(make):
        def one(k, c):
            make(lax.rem(me + k, n)).start()
            return c

        lax.fori_loop(1, n, one, 0)

    to_others(lambda dest: kv_send(dest, 1))

    wout_copy = pltpu.make_async_copy(wout_ref, wout, wout_sem)
    wout_copy.start()
    for s in range(slots):
        for copy in chunk_copies(s):
            copy.start()

    per = 4
    kv_per = 2
    q_tile = per * half_rows
    kv_tile = kv_per * rows
    scale2 = LOG2E * hd ** -0.5

    def arrive_kv(h):
        def one(src, c):
            @pl.when(src != me)
            def _():
                kv_recv(src, h).wait_recv()

            @pl.when(src == me)
            def _():
                kv_local(h).wait()

            kbuf[pl.ds(pl.multiple_of(src * rows, rows), rows), :] = kvr[src, h, 0:hd, :].T
            return c

        lax.fori_loop(0, n, one, 0)

    def arrive_q(u):
        def one(k, c):
            q_recv(lax.rem(me + k, n), u).wait_recv()
            return c

        lax.fori_loop(1, n, one, 0)
        q_local(u).wait()

    def attend(h, f):
        def one_tile(i, c):
            q_t = jnp.concatenate([qr[per * i + r, h, f] for r in range(per)], axis=1)

            def scores(j, q):
                k_blk = kbuf[pl.ds(pl.multiple_of(j * kv_tile, kv_tile), kv_tile), :]
                return jnp.dot(k_blk, q, preferred_element_type=jnp.float32)

            def values(j):
                return jnp.concatenate([kvr[kv_per * j + r, h, hd:2 * hd, :] for r in range(kv_per)], axis=1)

            def update(j, s, carry):
                m_new = jnp.max(s, axis=0, keepdims=True)
                if carry is not None:
                    m, l, o = carry
                    m_new = jnp.maximum(m, m_new)
                p = jnp.exp2((s - m_new) * scale2)
                l_new = jnp.sum(p, axis=0, keepdims=True)
                o_new = jnp.dot(values(j), p.astype(jnp.bfloat16), preferred_element_type=jnp.float32)
                if carry is not None:
                    alpha = jnp.exp2((m - m_new) * scale2)
                    l_new = alpha * l + l_new
                    o_new = alpha * o + o_new
                return m_new, l_new, o_new

            def masked(j, off, lane0):
                q = q_t[:, lane0:]
                s = scores(j, q)
                lane = lane0 + lax.broadcasted_iota(jnp.int32, s.shape, 1)
                query_pos = (lane // half_rows) * rows + f * half_rows + lane % half_rows
                key_pos = off + lax.broadcasted_iota(jnp.int32, s.shape, 0)
                return jnp.where(key_pos <= query_pos, s, -jnp.inf)

            diag = per // kv_per
            carry = update(diag * i, masked(diag * i, 0, 0), None)
            cut = q_tile // diag
            late = update(diag * i + 1, masked(diag * i + 1, kv_tile, cut), tuple(v[:, cut:] for v in carry))
            carry = tuple(jnp.concatenate([v[:, :cut], w], axis=1) for v, w in zip(carry, late))
            m, l, o = lax.fori_loop(0, diag * i, lambda j, cr: update(j, scores(j, q_t), cr), carry)
            out = (o / l).astype(jnp.bfloat16)
            for r in range(per):
                dest = per * i + r
                osend[f, dest, h] = out[:, r * half_rows:(r + 1) * half_rows]
                if h == hpd - 1:
                    @pl.when(dest != me)
                    def _():
                        o_send(dest, f).start()

                    @pl.when(dest == me)
                    def _():
                        o_local(f).start()
            return c

        lax.fori_loop(0, n // per, one_tile, 0)

    arrive_q(0)
    to_others(lambda dest: q_send(dest, 1))
    to_others(lambda dest: q_send(dest, 2))
    arrive_kv(0)
    attend(0, 0)
    attend(0, 1)
    arrive_kv(1)
    arrive_q(1)
    attend(1, 0)
    arrive_q(2)
    attend(1, 1)
    wout_copy.wait()

    def y_send(f):
        return remote(yn.at[f, 0], yn.at[f, 1], y_ss.at[f], y_rs.at[f], partner)

    def z_send(f):
        return remote(acc.at[f, 1], zrecv.at[f], z_ss.at[f], z_rs.at[f], partner)

    for f in range(HALVES):
        r0 = f * half_rows

        def arrive_o(k, c):
            o_recv(lax.rem(me + k, n), f).wait_recv()
            return c

        lax.fori_loop(1, n, arrive_o, 0)
        o_local(f).wait()
        o_rows = orecv[f].reshape(inner, half_rows).T
        mixed = jnp.dot(o_rows, wout[...], preferred_element_type=jnp.float32)
        y = (x_ref[r0:r0 + half_rows, :].astype(jnp.float32) + mixed).astype(jnp.bfloat16)
        ybuf[r0:r0 + half_rows, :] = y
        yn[f, 0] = rms_norm(y, gm_ref[...])
        y_send(f).start()
        acc[f] = jnp.zeros_like(acc[f])
        y_send(f).wait()

        def one_chunk(c, carry):
            s = f * nchunks + c
            slot = lax.rem(s, slots)
            cg, cu, cd = chunk_copies(s)
            y_all = yn[f].reshape(2 * half_rows, width)
            cg.wait()
            gate = jnp.dot(y_all, wg[slot], preferred_element_type=jnp.float32)
            cu.wait()
            up = jnp.dot(y_all, wu[slot], preferred_element_type=jnp.float32)
            hidden = (gate / (1.0 + jnp.exp(-gate)) * up).astype(jnp.bfloat16)
            cd.wait()
            part = jnp.dot(hidden, wd[slot], preferred_element_type=jnp.float32)
            acc[f] += part.reshape(2, half_rows, width)

            @pl.when(s + slots < HALVES * nchunks)
            def _():
                for copy in chunk_copies(s + slots):
                    copy.start()
            return carry

        lax.fori_loop(0, nchunks, one_chunk, 0)
        z_send(f).start()

    for f in range(HALVES):
        r0 = f * half_rows
        z_send(f).wait()
        total = acc[f, 0] + zrecv[f]
        z_ref[r0:r0 + half_rows, :] = (ybuf[r0:r0 + half_rows, :].astype(jnp.float32) + total).astype(jnp.bfloat16)

    def drain(k, c):
        other = lax.rem(me + k, n)
        for h in range(hpd):
            kv_send(other, h).wait_send()
        for u in range(3):
            q_send(other, u).wait_send()
        for f in range(HALVES):
            o_send(other, f).wait_send()
        return c

    lax.fori_loop(1, n, drain, 0)


def solution(mesh):
    n = mesh.shape['seq']

    def local_layer(x_blk, g_attn, w_qkv, w_out, g_mlp, w_gate, w_up, w_down):
        n_heads, hd, width = w_out.shape
        rows = x_blk.shape[0]
        hpd = n_heads // n
        member = lax.axis_index('seq')
        cos_t, sin_t = rope_tables_t(member * rows + jnp.arange(rows), hd)
        group = 1
        while (group * hpd * hd) % 128:
            group *= 2
        chunk, slots = 512, 2
        half = rows // HALVES
        bf16, f32 = jnp.bfloat16, jnp.float32
        vmem = pl.BlockSpec(memory_space=pltpu.VMEM)
        hbm = pl.BlockSpec(memory_space=pl.ANY)
        dma = pltpu.SemaphoreType.DMA
        return pl.pallas_call(
            functools.partial(layer_kernel, n, hpd, hd, group, chunk, slots),
            out_shape=jax.ShapeDtypeStruct(x_blk.shape, bf16),
            in_specs=[vmem] * 5 + [hbm] * 5,
            out_specs=vmem,
            scratch_shapes=[
                pltpu.VMEM((n_heads * hd, width), bf16),
                pltpu.VMEM((rows, width), bf16),
                pltpu.VMEM((n, hpd, 2 * hd, rows), bf16),
                pltpu.VMEM((n, hpd, 2 * hd, rows), bf16),
                pltpu.VMEM((n, hpd, HALVES, hd, half), bf16),
                pltpu.VMEM((n, hpd, HALVES, hd, half), bf16),
                pltpu.VMEM((n * rows, hd), bf16),
                pltpu.VMEM((HALVES, n, hpd, hd, half), bf16),
                pltpu.VMEM((HALVES, n, hpd, hd, half), bf16),
                pltpu.VMEM((HALVES, 2, half, width), bf16),
                pltpu.VMEM((rows, width), bf16),
                pltpu.VMEM((HALVES, 2, half, width), f32),
                pltpu.VMEM((HALVES, half, width), f32),
                pltpu.VMEM((slots, width, chunk), bf16),
                pltpu.VMEM((slots, width, chunk), bf16),
                pltpu.VMEM((slots, chunk, width), bf16),
                dma((4,)), dma, dma((3, slots)),
                dma((n, hpd)), dma((n, hpd)), dma((n, 3)), dma((n, 3)), dma((HALVES, n)), dma((HALVES, n)),
                dma((HALVES,)), dma((HALVES,)), dma((HALVES,)), dma((HALVES,)),
            ],
            compiler_params=pltpu.CompilerParams(collective_id=0, has_side_effects=True, vmem_limit_bytes=67043328),
            name='layer',
        )(x_blk, g_attn[None, :], g_mlp[None, :], cos_t, sin_t, w_qkv, w_out.reshape(n_heads * hd, width), w_gate, w_up, w_down)

    row_spec = P(('data', 'seq'), None)
    return jax.shard_map(local_layer, mesh=mesh, in_specs=(row_spec, P(), P(), P(), P(), P(), P(), P()), out_specs=row_spec, check_vma=False)
```

```python
import functools
import math

import jax
import jax.numpy as jnp
from jax import lax
from jax.experimental import pallas as pl
from jax.experimental.pallas import tpu as pltpu
from jax.sharding import PartitionSpec as P

ROPE_BASE = 10000
LOG2E = math.log2(math.e)
HALVES = 2
MESH = pl.DeviceIdType.MESH


def rms_norm(row_vals, gain_vec):
    rows_f32 = row_vals.astype(jnp.float32)
    inv_rms = lax.rsqrt(jnp.mean(rows_f32 * rows_f32, axis=-1, keepdims=True) + 1e-5)
    return (rows_f32 * inv_rms * gain_vec).astype(jnp.bfloat16)


def rope_tables_t(positions, head_dim):
    inv_freq = 1.0 / (ROPE_BASE ** (jnp.arange(0, head_dim, 2, dtype=jnp.float32) / head_dim))
    angles = inv_freq[:, None] * positions.astype(jnp.float32)[None, :]
    return jnp.cos(angles), jnp.sin(angles)


def layer_kernel(n, hpd, hd, group, chunk, slots,
                 xin_ref, ga_ref, gm_ref, cos_ref, sin_ref, wqkv_ref, wout_ref, wg_ref, wu_ref, wd_ref, z_ref,
                 x_ref, wout, xn, kvs, kvr, qs, qr, kbuf, osend, orecv, yn, hidden, zown, zsend, zrecv, wbuf,
                 x_sem, stage_sem, wout_sem, w_sem, kv_ss, kv_rs, q_ss, q_rs, o_ss, o_rs, y_ss, y_rs, z_ss, z_rs):
    rows, width = x_ref.shape
    half_rows = rows // HALVES
    inner = n * hpd * hd
    gcols = group * hpd * hd
    ngroups = n // group
    stages = width // gcols
    ff_half = wg_ref.shape[1] // 2
    nup = ff_half // chunk
    ndown = width // chunk
    nsteps = nup + ndown
    me = lax.axis_index('seq')
    core = lax.rem(me, 2)
    partner = me + 1 - 2 * core
    mygrp = me // group

    def grp_of(g):
        return lax.rem(mygrp + ngroups // 2 + g, ngroups)

    def tile_copy(s, t, g):
        col = pl.multiple_of(t * inner + grp_of(g) * gcols, 128)
        slot = pl.multiple_of(lax.rem(s, stages) * gcols, 128)
        return pltpu.make_async_copy(wqkv_ref.at[:, pl.ds(col, gcols)], wout.at[:, pl.ds(slot, gcols)],
                                     stage_sem.at[lax.rem(s, stages)])

    def start_tile(s):
        @pl.when(s < 2 * ngroups)
        def _():
            tile_copy(s, 1 + lax.rem(s, 2), s // 2).start()

        @pl.when(jnp.logical_and(s >= 2 * ngroups, s < 3 * ngroups))
        def _():
            tile_copy(s, 0, s - 2 * ngroups).start()

    def up_copies(c, slot):
        ff = pl.multiple_of(core * ff_half + c * chunk, 128)
        return (pltpu.make_async_copy(wg_ref.at[:, pl.ds(ff, chunk)], wbuf.at[slot, 0:width], w_sem.at[slot, 0]),
                pltpu.make_async_copy(wu_ref.at[:, pl.ds(ff, chunk)], wbuf.at[slot, width:2 * width], w_sem.at[slot, 1]))

    def down_copies(c, slot):
        col = pl.multiple_of(c * chunk, 128)
        return tuple(pltpu.make_async_copy(wd_ref.at[pl.ds(core * ff_half + p * width, width), pl.ds(col, chunk)],
                                           wbuf.at[slot, p * width:(p + 1) * width], w_sem.at[slot, p]) for p in range(2))

    def start_step(s):
        c = lax.rem(s, nsteps)
        slot = lax.rem(s, slots)

        @pl.when(jnp.logical_and(c < nup, s < HALVES * nsteps))
        def _():
            for copy in up_copies(c, slot):
                copy.start()

        @pl.when(jnp.logical_and(c >= nup, s < HALVES * nsteps))
        def _():
            for copy in down_copies(c - nup, slot):
                copy.start()

    x_copy = pltpu.make_async_copy(xin_ref, x_ref, x_sem)
    x_copy.start()
    for s in range(stages):
        start_tile(s)

    barrier = pltpu.get_barrier_semaphore()

    def greet(k, c):
        pl.semaphore_signal(barrier, inc=1, device_id={'seq': lax.rem(me + k, n)}, device_id_type=MESH)
        return c

    lax.fori_loop(1, n, greet, 0)
    def gain(ref):
        return jnp.concatenate([ref[r:r + 1, :] for r in range(ref.shape[0])], axis=1)

    x_copy.wait()
    xn[...] = rms_norm(x_ref[...], gain(ga_ref))

    def remote(src, dst, ssem, rsem, dest):
        return pltpu.make_async_remote_copy(src_ref=src, dst_ref=dst, send_sem=ssem, recv_sem=rsem,
                                            device_id={'seq': dest}, device_id_type=MESH)

    def kv_send(dest, h):
        return remote(kvs.at[dest, h], kvr.at[me, h], kv_ss.at[dest, h], kv_rs.at[me, h], dest)

    def kv_recv(src, h):
        return remote(kvs.at[src, h], kvr.at[src, h], kv_ss.at[src, h], kv_rs.at[src, h], src)

    def kv_local(h):
        return pltpu.make_async_copy(kvs.at[me, h], kvr.at[me, h], kv_rs.at[me, h])

    def q_send(dest, u):
        src, dst = (qs.at[dest, 0], qr.at[me, 0]) if u == 0 else (qs.at[dest, 1, u - 1], qr.at[me, 1, u - 1])
        return remote(src, dst, q_ss.at[dest, u], q_rs.at[me, u], dest)

    def q_recv(src, u):
        a, b = (qs.at[src, 0], qr.at[src, 0]) if u == 0 else (qs.at[src, 1, u - 1], qr.at[src, 1, u - 1])
        return remote(a, b, q_ss.at[src, u], q_rs.at[src, u], src)

    def q_local(u):
        src, dst = (qs.at[me, 0], qr.at[me, 0]) if u == 0 else (qs.at[me, 1, u - 1], qr.at[me, 1, u - 1])
        return pltpu.make_async_copy(src, dst, q_rs.at[me, u])

    def o_send(dest, f):
        return remote(osend.at[f, dest], orecv.at[f, me], o_ss.at[f, dest], o_rs.at[f, me], dest)

    def o_recv(src, f):
        return remote(osend.at[f, src], orecv.at[f, src], o_ss.at[f, src], o_rs.at[f, src], src)

    def o_local(f):
        return pltpu.make_async_copy(osend.at[f, me], orecv.at[f, me], o_rs.at[f, me])

    def project(s):
        start = pl.multiple_of(lax.rem(s, stages) * gcols, 128)
        out = jnp.dot(xn[...], wout[:, pl.ds(start, gcols)], preferred_element_type=jnp.float32)
        start_tile(s + stages)
        return out.T

    def rope(u):
        lo, hi = u[:hd // 2], u[hd // 2:]
        cos, sin = cos_ref[...], sin_ref[...]
        return jnp.concatenate([lo * cos - hi * sin, hi * cos + lo * sin], axis=0)

    def send_group(g, make):
        def one(k, c):
            dest = grp_of(g) * group + k

            @pl.when(dest != me)
            def _():
                make(dest).start()
            return c

        lax.fori_loop(0, group, one, 0)

    def project_kv(g, c):
        for t in (0, 1):
            tile_copy(2 * g + t, 1 + t, g).wait()
            out = project(2 * g + t)
            for k in range(group * hpd):
                u = out[k * hd:(k + 1) * hd]
                if t == 0:
                    u = rope(u)
                kvs[grp_of(g) * group + k // hpd, k % hpd, t * hd:(t + 1) * hd, :] = u.astype(jnp.bfloat16)
        @pl.when(g == 0)
        def _():
            pl.semaphore_wait(barrier, n - 1)

        send_group(g, lambda dest: kv_send(dest, 0))
        return c

    lax.fori_loop(0, ngroups, project_kv, 0)
    kv_local(0).start()
    kv_local(1).start()

    def project_q(g, c):
        s = 2 * ngroups + g
        tile_copy(s, 0, g).wait()
        out = project(s)
        for k in range(group * hpd):
            u = rope(out[k * hd:(k + 1) * hd]).astype(jnp.bfloat16)
            for f in range(HALVES):
                qs[grp_of(g) * group + k // hpd, k % hpd, f] = u[:, f * half_rows:(f + 1) * half_rows]
        send_group(g, lambda dest: q_send(dest, 0))
        return c

    lax.fori_loop(0, ngroups, project_q, 0)
    for u in range(3):
        q_local(u).start()

    def to_others(make):
        def one(k, c):
            make(lax.rem(me + k, n)).start()
            return c

        lax.fori_loop(1, n, one, 0)

    to_others(lambda dest: kv_send(dest, 1))

    wout_copy = pltpu.make_async_copy(wout_ref, wout, wout_sem)
    wout_copy.start()
    for s in range(slots):
        start_step(s)

    per = 4
    kv_per = 2
    q_tile = per * half_rows
    kv_tile = kv_per * rows
    scale2 = LOG2E * hd ** -0.5

    def arrive_kv(h):
        def one(src, c):
            @pl.when(src != me)
            def _():
                kv_recv(src, h).wait_recv()

            @pl.when(src == me)
            def _():
                kv_local(h).wait()

            kbuf[pl.ds(pl.multiple_of(src * rows, rows), rows), :] = kvr[src, h, 0:hd, :].T
            return c

        lax.fori_loop(0, n, one, 0)

    def arrive_q(u):
        def one(k, c):
            q_recv(lax.rem(me + k, n), u).wait_recv()
            return c

        lax.fori_loop(1, n, one, 0)
        q_local(u).wait()

    def attend(h, f):
        def one_tile(i, c):
            q_t = jnp.concatenate([qr[per * i + r, h, f] for r in range(per)], axis=1)

            def scores(j, q, blocks=kv_per):
                size = blocks * rows
                k_blk = kbuf[pl.ds(pl.multiple_of(j * size, size), size), :]
                return jnp.dot(k_blk, q, preferred_element_type=jnp.float32)

            def values(j, blocks):
                return jnp.concatenate([kvr[blocks * j + r, h, hd:2 * hd, :] for r in range(blocks)], axis=1)

            def update(j, s, carry, blocks=kv_per):
                m_new = jnp.max(s, axis=0, keepdims=True)
                if carry is not None:
                    m, l, o = carry
                    m_new = jnp.maximum(m, m_new)
                p = jnp.exp2((s - m_new) * scale2)
                l_new = jnp.sum(p, axis=0, keepdims=True)
                o_new = jnp.dot(values(j, blocks), p.astype(jnp.bfloat16), preferred_element_type=jnp.float32)
                if carry is not None:
                    alpha = jnp.exp2((m - m_new) * scale2)
                    l_new = alpha * l + l_new
                    o_new = alpha * o + o_new
                return m_new, l_new, o_new

            def masked(j, off, lane0):
                q = q_t[:, lane0:]
                s = scores(j, q)
                lane = lane0 + lax.broadcasted_iota(jnp.int32, s.shape, 1)
                query_pos = (lane // half_rows) * rows + f * half_rows + lane % half_rows
                key_pos = off + lax.broadcasted_iota(jnp.int32, s.shape, 0)
                return jnp.where(key_pos <= query_pos, s, -jnp.inf)

            diag = per // kv_per
            carry = update(diag * i, masked(diag * i, 0, 0), None)
            cut = q_tile // diag
            late = update(diag * i + 1, masked(diag * i + 1, kv_tile, cut), tuple(v[:, cut:] for v in carry))
            carry = tuple(jnp.concatenate([v[:, :cut], w], axis=1) for v, w in zip(carry, late))
            m, l, o = lax.fori_loop(0, i, lambda j, cr: update(j, scores(j, q_t, per), cr, per), carry)
            out = (o / l).astype(jnp.bfloat16)
            for r in range(per):
                dest = per * i + r
                osend[f, dest, h] = out[:, r * half_rows:(r + 1) * half_rows]
                if h == hpd - 1:
                    @pl.when(dest != me)
                    def _():
                        o_send(dest, f).start()

                    @pl.when(dest == me)
                    def _():
                        o_local(f).start()
            return c

        lax.fori_loop(0, n // per, one_tile, 0)

    arrive_q(0)
    to_others(lambda dest: q_send(dest, 1))
    to_others(lambda dest: q_send(dest, 2))
    arrive_kv(0)
    attend(0, 0)
    attend(0, 1)
    arrive_kv(1)
    arrive_q(1)
    attend(1, 0)
    arrive_q(2)
    attend(1, 1)
    wout_copy.wait()

    def y_send(f):
        return remote(yn.at[f, 0], yn.at[f, 1], y_ss.at[f], y_rs.at[f], partner)

    def z_send(f, c):
        return remote(zsend.at[c], zrecv.at[f, c], z_ss.at[f, c], z_rs.at[f, c], partner)

    def out_projection(f):
        r0 = f * half_rows

        def arrive_o(k, c):
            o_recv(lax.rem(me + k, n), f).wait_recv()
            return c

        lax.fori_loop(1, n, arrive_o, 0)
        o_local(f).wait()
        o_rows = orecv[f].reshape(inner, half_rows).T
        mixed = jnp.dot(o_rows, wout[...], preferred_element_type=jnp.float32)
        y = (x_ref[r0:r0 + half_rows, :].astype(jnp.float32) + mixed).astype(jnp.bfloat16)
        x_ref[r0:r0 + half_rows, :] = y
        yn[f, 0] = rms_norm(y, gain(gm_ref))
        y_send(f).start()

    def gate_up(f):
        def one(c, carry):
            s = f * nsteps + c
            slot = lax.rem(s, slots)
            for copy in up_copies(c, slot):
                copy.wait()
            y_all = yn[f].reshape(2 * half_rows, width)
            gate = jnp.dot(y_all, wbuf[slot, 0:width], preferred_element_type=jnp.float32)
            up = jnp.dot(y_all, wbuf[slot, width:2 * width], preferred_element_type=jnp.float32)
            hidden[:, pl.ds(pl.multiple_of(c * chunk, 128), chunk)] = (gate / (1.0 + jnp.exp(-gate)) * up).astype(jnp.bfloat16)
            start_step(s + slots)
            return carry

        lax.fori_loop(0, nup, one, 0)

    def down(f):
        def one(c, carry):
            s = f * nsteps + nup + c
            slot = lax.rem(s, slots)
            for copy in down_copies(c, slot):
                copy.wait()
            part = jnp.dot(hidden[...], wbuf[slot], preferred_element_type=jnp.float32)
            zsend[c] = part[half_rows:]
            z_send(f, c).start()
            zown[c] = part[:half_rows]
            start_step(s + slots)
            return carry

        lax.fori_loop(0, ndown, one, 0)

    def finish(f):
        r0 = f * half_rows
        for c in range(ndown):
            z_send(f, c).wait()
            total = zown[c] + zrecv[f, c]
            cols = slice(c * chunk, (c + 1) * chunk)
            z_ref[r0:r0 + half_rows, cols] = (x_ref[r0:r0 + half_rows, cols].astype(jnp.float32) + total).astype(jnp.bfloat16)

    out_projection(0)
    y_send(0).wait()
    gate_up(0)
    out_projection(1)
    down(0)
    y_send(1).wait()
    gate_up(1)
    finish(0)
    down(1)
    finish(1)

    def drain(k, c):
        other = lax.rem(me + k, n)
        for h in range(hpd):
            kv_send(other, h).wait_send()
        for u in range(3):
            q_send(other, u).wait_send()
        for f in range(HALVES):
            o_send(other, f).wait_send()
        return c

    lax.fori_loop(1, n, drain, 0)


def solution(mesh):
    n = mesh.shape['seq']

    def local_layer(x_blk, g_attn, w_qkv, w_out, g_mlp, w_gate, w_up, w_down):
        n_heads, hd, width = w_out.shape
        rows = x_blk.shape[0]
        hpd = n_heads // n
        member = lax.axis_index('seq')
        cos_t, sin_t = rope_tables_t(member * rows + jnp.arange(rows), hd)
        group = 1
        while (group * hpd * hd) % 128:
            group *= 2
        chunk, slots = 512, 4
        half = rows // HALVES
        bf16, f32 = jnp.bfloat16, jnp.float32
        vmem = pl.BlockSpec(memory_space=pltpu.VMEM)
        hbm = pl.BlockSpec(memory_space=pl.ANY)
        dma = pltpu.SemaphoreType.DMA
        return pl.pallas_call(
            functools.partial(layer_kernel, n, hpd, hd, group, chunk, slots),
            out_shape=jax.ShapeDtypeStruct(x_blk.shape, bf16),
            in_specs=[hbm] + [vmem] * 4 + [hbm] * 5,
            out_specs=vmem,
            scratch_shapes=[
                pltpu.VMEM((rows, width), bf16),
                pltpu.VMEM((n_heads * hd, width), bf16),
                pltpu.VMEM((rows, width), bf16),
                pltpu.VMEM((n, hpd, 2 * hd, rows), bf16),
                pltpu.VMEM((n, hpd, 2 * hd, rows), bf16),
                pltpu.VMEM((n, hpd, HALVES, hd, half), bf16),
                pltpu.VMEM((n, hpd, HALVES, hd, half), bf16),
                pltpu.VMEM((n * rows, hd), bf16),
                pltpu.VMEM((HALVES, n, hpd, hd, half), bf16),
                pltpu.VMEM((HALVES, n, hpd, hd, half), bf16),
                pltpu.VMEM((HALVES, 2, half, width), bf16),
                pltpu.VMEM((rows, w_down.shape[0] // 2), bf16),
                pltpu.VMEM((width // chunk, half, chunk), f32),
                pltpu.VMEM((width // chunk, half, chunk), f32),
                pltpu.VMEM((HALVES, width // chunk, half, chunk), f32),
                pltpu.VMEM((slots, 2 * width, chunk), bf16),
                dma, dma((4,)), dma, dma((slots, 2)),
                dma((n, hpd)), dma((n, hpd)), dma((n, 3)), dma((n, 3)), dma((HALVES, n)), dma((HALVES, n)),
                dma((HALVES,)), dma((HALVES,)), dma((HALVES, width // chunk)), dma((HALVES, width // chunk)),
            ],
            compiler_params=pltpu.CompilerParams(collective_id=0, has_side_effects=True, vmem_limit_bytes=67043328),
            name='layer',
        )(x_blk, g_attn.reshape(-1, 128), g_mlp.reshape(-1, 128), cos_t, sin_t, w_qkv, w_out.reshape(n_heads * hd, width), w_gate, w_up, w_down)

    row_spec = P(('data', 'seq'), None)
    return jax.shard_map(local_layer, mesh=mesh, in_specs=(row_spec, P(), P(), P(), P(), P(), P(), P()), out_specs=row_spec, check_vma=False)
```

```python
import functools
import math

import jax
import jax.numpy as jnp
from jax import lax
from jax.experimental import pallas as pl
from jax.experimental.pallas import tpu as pltpu
from jax.sharding import PartitionSpec as P

ROPE_BASE = 10000
LOG2E = math.log2(math.e)
HALVES = 2
MESH = pl.DeviceIdType.MESH


def rms_norm(row_vals, gain_vec):
    rows_f32 = row_vals.astype(jnp.float32)
    inv_rms = lax.rsqrt(jnp.mean(rows_f32 * rows_f32, axis=-1, keepdims=True) + 1e-5)
    return (rows_f32 * inv_rms * gain_vec).astype(jnp.bfloat16)


def rope_tables_t(positions, head_dim):
    inv_freq = 1.0 / (ROPE_BASE ** (jnp.arange(0, head_dim, 2, dtype=jnp.float32) / head_dim))
    angles = inv_freq[:, None] * positions.astype(jnp.float32)[None, :]
    return jnp.cos(angles), jnp.sin(angles)


def layer_kernel(n, hpd, hd, group, chunk, slots,
                 xin_ref, gain_refs, gainm_refs, cosin_ref, sinin_ref, wqkv_ref, wout_ref, wg_ref, wu_ref, wd_ref, z_ref,
                 x_ref, ga_ref, gm_ref, cos_ref, sin_ref, wout, kvs, kvr, qs, qr, kbuf, osend, orecv, yn, hidden, zown, zsend, zrecv, wbuf,
                 in_sem, stage_sem, wout_sem, w_sem, kv_ss, kv_rs, q_ss, q_rs, o_ss, o_rs, y_ss, y_rs, z_ss, z_rs):
    rows, width = x_ref.shape
    half_rows = rows // HALVES
    inner = n * hpd * hd
    gcols = group * hpd * hd
    ngroups = n // group
    stages = width // gcols
    ff_half = wg_ref.shape[1] // 2
    nup = ff_half // chunk
    ndown = width // chunk
    nsteps = nup + ndown
    me = lax.axis_index('seq')
    core = lax.rem(me, 2)
    partner = me + 1 - 2 * core
    mygrp = me // group

    order = sorted(range(ngroups), key=lambda d: -min(d, ngroups - d))

    def grp_of(g):
        off = 0
        for i, d in enumerate(order):
            off = jnp.where(g == i, d, off)
        return lax.rem(mygrp + off, ngroups)

    def tile_copy(s, t, g):
        col = pl.multiple_of(t * inner + grp_of(g) * gcols, 128)
        slot = pl.multiple_of(lax.rem(s, stages) * gcols, 128)
        return pltpu.make_async_copy(wqkv_ref.at[:, pl.ds(col, gcols)], wout.at[:, pl.ds(slot, gcols)],
                                     stage_sem.at[lax.rem(s, stages)])

    def start_tile(s):
        @pl.when(s < 2 * ngroups)
        def _():
            tile_copy(s, 1 + lax.rem(s, 2), s // 2).start()

        @pl.when(jnp.logical_and(s >= 2 * ngroups, s < 3 * ngroups))
        def _():
            tile_copy(s, 0, s - 2 * ngroups).start()

    def up_copies(c, slot):
        ff = pl.multiple_of(core * ff_half + c * chunk, 128)
        return (pltpu.make_async_copy(wg_ref.at[:, pl.ds(ff, chunk)], wbuf.at[slot, 0:width], w_sem.at[slot, 0]),
                pltpu.make_async_copy(wu_ref.at[:, pl.ds(ff, chunk)], wbuf.at[slot, width:2 * width], w_sem.at[slot, 1]))

    def down_copies(c, slot):
        col = pl.multiple_of(c * chunk, 128)
        return tuple(pltpu.make_async_copy(wd_ref.at[pl.ds(core * ff_half + p * width, width), pl.ds(col, chunk)],
                                           wbuf.at[slot, p * width:(p + 1) * width], w_sem.at[slot, p]) for p in range(2))

    def start_up(c):
        for copy in up_copies(c, lax.rem(c, slots)):
            copy.start()

    def down_slot(c):
        return slots - 1 - lax.rem(c, slots)

    def start_down(c):
        for copy in down_copies(c, down_slot(c)):
            copy.start()

    inputs = [pltpu.make_async_copy(src, dst, in_sem.at[i]) for i, (src, dst) in enumerate(
        [(xin_ref, x_ref), (gain_refs, ga_ref), (cosin_ref, cos_ref), (sinin_ref, sin_ref), (gainm_refs, gm_ref)])]
    inputs[0].start()
    inputs[1].start()
    for s in range(stages):
        start_tile(s)
    for copy in inputs[2:]:
        copy.start()

    barrier = pltpu.get_barrier_semaphore()

    def greet(k, c):
        pl.semaphore_signal(barrier, inc=1, device_id={'seq': lax.rem(me + k, n)}, device_id_type=MESH)
        return c

    lax.fori_loop(1, n, greet, 0)
    def gain(ref):
        return jnp.concatenate([ref[r:r + 1, :] for r in range(ref.shape[0])], axis=1)

    inputs[0].wait()
    inputs[1].wait()
    yn[1] = rms_norm(x_ref[...], gain(ga_ref)).reshape(2, half_rows, width)
    for copy in inputs[2:]:
        copy.wait()

    def remote(src, dst, ssem, rsem, dest):
        return pltpu.make_async_remote_copy(src_ref=src, dst_ref=dst, send_sem=ssem, recv_sem=rsem,
                                            device_id={'seq': dest}, device_id_type=MESH)

    def kv_part(ref, u):
        return ref.at[1] if u == 2 else ref.at[0, u * hd:(u + 1) * hd]

    def kv_send(dest, u):
        return remote(kv_part(kvs.at[dest], u), kv_part(kvr.at[me], u), kv_ss.at[dest, u], kv_rs.at[me, u], dest)

    def kv_recv(src, u):
        return remote(kv_part(kvs.at[src], u), kv_part(kvr.at[src], u), kv_ss.at[src, u], kv_rs.at[src, u], src)

    def kv_local(u):
        return pltpu.make_async_copy(kv_part(kvs.at[me], u), kv_part(kvr.at[me], u), kv_rs.at[me, u])

    def q_send(dest, u):
        src, dst = (qs.at[dest, 0], qr.at[me, 0]) if u == 0 else (qs.at[dest, 1, u - 1], qr.at[me, 1, u - 1])
        return remote(src, dst, q_ss.at[dest, u], q_rs.at[me, u], dest)

    def q_recv(src, u):
        a, b = (qs.at[src, 0], qr.at[src, 0]) if u == 0 else (qs.at[src, 1, u - 1], qr.at[src, 1, u - 1])
        return remote(a, b, q_ss.at[src, u], q_rs.at[src, u], src)

    def q_local(u):
        src, dst = (qs.at[me, 0], qr.at[me, 0]) if u == 0 else (qs.at[me, 1, u - 1], qr.at[me, 1, u - 1])
        return pltpu.make_async_copy(src, dst, q_rs.at[me, u])

    def o_send(dest, f):
        return remote(osend.at[f, dest], orecv.at[f, me], o_ss.at[f, dest], o_rs.at[f, me], dest)

    def o_recv(src, f):
        return remote(osend.at[f, src], orecv.at[f, src], o_ss.at[f, src], o_rs.at[f, src], src)

    def o_local(f):
        return pltpu.make_async_copy(osend.at[f, me], orecv.at[f, me], o_rs.at[f, me])

    def project(s):
        start = pl.multiple_of(lax.rem(s, stages) * gcols, 128)
        out = jnp.dot(yn[1].reshape(rows, width), wout[:, pl.ds(start, gcols)], preferred_element_type=jnp.float32)
        start_tile(s + stages)
        return out.T

    def rope(u):
        lo, hi = u[:hd // 2], u[hd // 2:]
        cos, sin = cos_ref[...], sin_ref[...]
        return jnp.concatenate([lo * cos - hi * sin, hi * cos + lo * sin], axis=0)

    def send_group(g, make):
        def one(k, c):
            dest = grp_of(g) * group + k

            @pl.when(dest != me)
            def _():
                make(dest).start()
            return c

        lax.fori_loop(0, group, one, 0)

    def project_kv(g, c):
        for t in (0, 1):
            tile_copy(2 * g + t, 1 + t, g).wait()
            out = project(2 * g + t)
            for k in range(group * hpd):
                u = out[k * hd:(k + 1) * hd]
                if t == 0:
                    u = rope(u)
                kvs[grp_of(g) * group + k // hpd, k % hpd, t * hd:(t + 1) * hd, :] = u.astype(jnp.bfloat16)
            if t == 0:
                @pl.when(g == 0)
                def _():
                    pl.semaphore_wait(barrier, n - 1)

            send_group(g, lambda dest: kv_send(dest, t))
        return c

    lax.fori_loop(0, ngroups, project_kv, 0)
    for u in range(3):
        kv_local(u).start()

    def project_q(g, c):
        s = 2 * ngroups + g
        tile_copy(s, 0, g).wait()
        out = project(s)
        for k in range(group * hpd):
            u = rope(out[k * hd:(k + 1) * hd]).astype(jnp.bfloat16)
            for f in range(HALVES):
                qs[grp_of(g) * group + k // hpd, k % hpd, f] = u[:, f * half_rows:(f + 1) * half_rows]
        send_group(g, lambda dest: q_send(dest, 0))
        return c

    lax.fori_loop(0, ngroups, project_q, 0)
    for u in range(3):
        q_local(u).start()

    def to_others(make):
        def one(k, c):
            make(lax.rem(me + k, n)).start()
            return c

        lax.fori_loop(1, n, one, 0)

    to_others(lambda dest: kv_send(dest, 2))

    wout_copy = pltpu.make_async_copy(wout_ref, wout, wout_sem)
    wout_copy.start()
    for c in range(slots):
        start_up(c)

    per = 4
    kv_per = 2
    q_tile = per * half_rows
    kv_tile = kv_per * rows
    scale2 = LOG2E * hd ** -0.5

    def arrive_kv(h):
        def one(src, c):
            for u in ((0, 1) if h == 0 else (2,)):
                @pl.when(src != me)
                def _():
                    kv_recv(src, u).wait_recv()

                @pl.when(src == me)
                def _():
                    kv_local(u).wait()

            kbuf[pl.ds(pl.multiple_of(src * rows, rows), rows), :] = kvr[src, h, 0:hd, :].T
            return c

        lax.fori_loop(0, n, one, 0)

    def arrive_q(u):
        def one(k, c):
            q_recv(lax.rem(me + k, n), u).wait_recv()
            return c

        lax.fori_loop(1, n, one, 0)
        q_local(u).wait()

    def attend(h, f):
        def one_tile(i, c):
            q_t = jnp.concatenate([qr[per * i + r, h, f] for r in range(per)], axis=1)

            def scores(j, q, blocks=kv_per):
                size = blocks * rows
                k_blk = kbuf[pl.ds(pl.multiple_of(j * size, size), size), :]
                return jnp.dot(k_blk, q, preferred_element_type=jnp.float32)

            def values(j, blocks):
                return jnp.concatenate([kvr[blocks * j + r, h, hd:2 * hd, :] for r in range(blocks)], axis=1)

            def update(j, s, carry, blocks=kv_per):
                m_new = jnp.max(s, axis=0, keepdims=True)
                if carry is not None:
                    m, l, o = carry
                    m_new = jnp.maximum(m, m_new)
                p = jnp.exp2((s - m_new) * scale2)
                l_new = jnp.sum(p, axis=0, keepdims=True)
                o_new = jnp.dot(values(j, blocks), p.astype(jnp.bfloat16), preferred_element_type=jnp.float32)
                if carry is not None:
                    alpha = jnp.exp2((m - m_new) * scale2)
                    l_new = alpha * l + l_new
                    o_new = alpha * o + o_new
                return m_new, l_new, o_new

            def masked(j, off, lane0):
                q = q_t[:, lane0:]
                s = scores(j, q)
                lane = lane0 + lax.broadcasted_iota(jnp.int32, s.shape, 1)
                query_pos = (lane // half_rows) * rows + f * half_rows + lane % half_rows
                key_pos = off + lax.broadcasted_iota(jnp.int32, s.shape, 0)
                return jnp.where(key_pos <= query_pos, s, -jnp.inf)

            diag = per // kv_per
            carry = update(diag * i, masked(diag * i, 0, 0), None)
            cut = q_tile // diag
            late = update(diag * i + 1, masked(diag * i + 1, kv_tile, cut), tuple(v[:, cut:] for v in carry))
            carry = tuple(jnp.concatenate([v[:, :cut], w], axis=1) for v, w in zip(carry, late))
            m, l, o = lax.fori_loop(0, i, lambda j, cr: update(j, scores(j, q_t, per), cr, per), carry)
            out = (o / l).astype(jnp.bfloat16)
            for r in range(per):
                dest = per * i + r
                osend[f, dest, h] = out[:, r * half_rows:(r + 1) * half_rows]
                if h == hpd - 1:
                    @pl.when(dest != me)
                    def _():
                        o_send(dest, f).start()

                    @pl.when(dest == me)
                    def _():
                        o_local(f).start()
            return c

        lax.fori_loop(0, n // per, one_tile, 0)

    arrive_q(0)
    to_others(lambda dest: q_send(dest, 1))
    to_others(lambda dest: q_send(dest, 2))
    arrive_kv(0)
    attend(0, 0)
    attend(0, 1)
    arrive_kv(1)
    arrive_q(1)
    attend(1, 0)
    arrive_q(2)
    attend(1, 1)
    wout_copy.wait()

    def y_send(f):
        return remote(yn.at[f, 0], yn.at[f, 1], y_ss.at[f], y_rs.at[f], partner)

    def z_send(c):
        return remote(zsend.at[c], zrecv.at[c], z_ss.at[c], z_rs.at[c], partner)

    def out_projection(f):
        r0 = f * half_rows

        def arrive_o(k, c):
            o_recv(lax.rem(me + k, n), f).wait_recv()
            return c

        lax.fori_loop(1, n, arrive_o, 0)
        o_local(f).wait()
        o_rows = orecv[f].reshape(inner, half_rows).T
        mixed = jnp.dot(o_rows, wout[...], preferred_element_type=jnp.float32)
        y = (x_ref[r0:r0 + half_rows, :].astype(jnp.float32) + mixed).astype(jnp.bfloat16)
        x_ref[r0:r0 + half_rows, :] = y
        yn[f, 0] = rms_norm(y, gain(gm_ref))
        y_send(f).start()

    def gate_up(f, first, last):
        def one(t, carry):
            c = t if f == 0 else nup - 1 - t
            slot = lax.rem(c, slots)
            if f == 0:
                for copy in up_copies(c, slot):
                    copy.wait()
            else:
                @pl.when(t >= slots)
                def _():
                    for copy in up_copies(c, slot):
                        copy.wait()
            y_all = yn[f].reshape(2 * half_rows, width)
            gate = jnp.dot(y_all, wbuf[slot, 0:width], preferred_element_type=jnp.float32)
            up = jnp.dot(y_all, wbuf[slot, width:2 * width], preferred_element_type=jnp.float32)
            cols = pl.ds(pl.multiple_of(c * chunk, 128), chunk)
            hidden[f, :, cols] = (gate / (1.0 + jnp.exp(-gate)) * up).astype(jnp.bfloat16)
            if f == 0:
                @pl.when(c + slots < nup)
                def _():
                    start_up(c + slots)
            else:
                @pl.when(c >= slots)
                def _():
                    start_up(c - slots)

                @pl.when(c < slots)
                def _():
                    start_down(slots - 1 - c)
            return carry

        lax.fori_loop(first, last, one, 0)

    def down(first, last):
        def one(c, carry):
            slot = down_slot(c)
            for copy in down_copies(c, slot):
                copy.wait()
            part = jnp.dot(hidden[...].reshape(HALVES * rows, ff_half), wbuf[slot], preferred_element_type=jnp.float32)
            part = part.reshape(HALVES, 2, half_rows, chunk)
            zsend[c] = part[:, 1]
            z_send(c).start()
            zown[c] = part[:, 0]

            @pl.when(c + slots < ndown)
            def _():
                start_down(c + slots)
            return carry

        lax.fori_loop(first, last, one, 0)

    def finish(c):
        z_send(c).wait()
        cols = slice(c * chunk, (c + 1) * chunk)
        total = (zown[c] + zrecv[c]).reshape(rows, chunk)
        z_ref[:, cols] = (x_ref[:, cols].astype(jnp.float32) + total).astype(jnp.bfloat16)

    out_projection(0)
    y_send(0).wait()
    gate_up(0, 0, nup - 2)
    out_projection(1)
    gate_up(0, nup - 2, nup)
    y_send(1).wait()
    gate_up(1, 0, nup)
    down(0, ndown - 1)
    for c in range(ndown - 2):
        finish(c)
    down(ndown - 1, ndown)
    for c in range(ndown - 2, ndown):
        finish(c)

    def drain(k, c):
        other = lax.rem(me + k, n)
        for u in range(3):
            kv_send(other, u).wait_send()
            q_send(other, u).wait_send()
        for f in range(HALVES):
            o_send(other, f).wait_send()
        return c

    lax.fori_loop(1, n, drain, 0)


def solution(mesh):
    n = mesh.shape['seq']

    def local_layer(x_blk, g_attn, w_qkv, w_out, g_mlp, w_gate, w_up, w_down):
        n_heads, hd, width = w_out.shape
        rows = x_blk.shape[0]
        hpd = n_heads // n
        member = lax.axis_index('seq')
        cos_t, sin_t = rope_tables_t(member * rows + jnp.arange(rows), hd)
        group = 1
        while (group * hpd * hd) % 128:
            group *= 2
        chunk, slots = 512, 3
        half = rows // HALVES
        bf16, f32 = jnp.bfloat16, jnp.float32
        vmem = pl.BlockSpec(memory_space=pltpu.VMEM)
        hbm = pl.BlockSpec(memory_space=pl.ANY)
        dma = pltpu.SemaphoreType.DMA
        return pl.pallas_call(
            functools.partial(layer_kernel, n, hpd, hd, group, chunk, slots),
            out_shape=pltpu.VMEM(x_blk.shape, bf16),
            in_specs=[hbm] * 10,
            out_specs=vmem,
            scratch_shapes=[
                pltpu.VMEM((rows, width), bf16),
                pltpu.VMEM((width // 128, 128), f32),
                pltpu.VMEM((width // 128, 128), f32),
                pltpu.VMEM((hd // 2, rows), f32),
                pltpu.VMEM((hd // 2, rows), f32),
                pltpu.VMEM((n_heads * hd, width), bf16),
                pltpu.VMEM((n, hpd, 2 * hd, rows), bf16),
                pltpu.VMEM((n, hpd, 2 * hd, rows), bf16),
                pltpu.VMEM((n, hpd, HALVES, hd, half), bf16),
                pltpu.VMEM((n, hpd, HALVES, hd, half), bf16),
                pltpu.VMEM((n * rows, hd), bf16),
                pltpu.VMEM((HALVES, n, hpd, hd, half), bf16),
                pltpu.VMEM((HALVES, n, hpd, hd, half), bf16),
                pltpu.VMEM((HALVES, 2, half, width), bf16),
                pltpu.VMEM((HALVES, rows, w_down.shape[0] // 2), bf16),
                pltpu.VMEM((width // chunk, HALVES, half, chunk), f32),
                pltpu.VMEM((width // chunk, HALVES, half, chunk), f32),
                pltpu.VMEM((width // chunk, HALVES, half, chunk), f32),
                pltpu.VMEM((slots, 2 * width, chunk), bf16),
                dma((5,)), dma((4,)), dma, dma((slots, 2)),
                dma((n, 3)), dma((n, 3)), dma((n, 3)), dma((n, 3)), dma((HALVES, n)), dma((HALVES, n)),
                dma((HALVES,)), dma((HALVES,)), dma((width // chunk,)), dma((width // chunk,)),
            ],
            compiler_params=pltpu.CompilerParams(collective_id=0, has_side_effects=True, vmem_limit_bytes=64 * 1000 * 1024),
            name='layer',
        )(x_blk, g_attn.reshape(-1, 128), g_mlp.reshape(-1, 128), cos_t, sin_t, w_qkv, w_out.reshape(n_heads * hd, width), w_gate, w_up, w_down)

    row_spec = P(('data', 'seq'), None)
    return jax.shard_map(local_layer, mesh=mesh, in_specs=(row_spec, P(), P(), P(), P(), P(), P(), P()), out_specs=row_spec, check_vma=False)
```

```python
import functools
import math

import jax
import jax.numpy as jnp
from jax import lax
from jax.experimental import pallas as pl
from jax.experimental.pallas import tpu as pltpu
from jax.sharding import PartitionSpec as P

ROPE_BASE = 10000
LOG2E = math.log2(math.e)
HALVES = 2
MESH = pl.DeviceIdType.MESH


def rms_norm(row_vals, gain_vec):
    rows_f32 = row_vals.astype(jnp.float32)
    inv_rms = lax.rsqrt(jnp.mean(rows_f32 * rows_f32, axis=-1, keepdims=True) + 1e-5)
    return (rows_f32 * inv_rms * gain_vec).astype(jnp.bfloat16)


def rope_tables_t(positions, head_dim):
    inv_freq = 1.0 / (ROPE_BASE ** (jnp.arange(0, head_dim, 2, dtype=jnp.float32) / head_dim))
    angles = inv_freq[:, None] * positions.astype(jnp.float32)[None, :]
    return jnp.cos(angles), jnp.sin(angles)


def layer_kernel(n, hpd, hd, group, chunk, slots,
                 xin_ref, gain_refs, gainm_refs, cosin_ref, sinin_ref, wqkv_ref, wout_ref, wg_ref, wu_ref, wd_ref, z_ref,
                 x_ref, ga_ref, gm_ref, cos_ref, sin_ref, wout, kvs, kvr, qs, qr, kbuf, sbuf, osend, orecv, yn, hidden, zown, zsend, zrecv, wbuf,
                 in_sem, stage_sem, wout_sem, w_sem, kv_ss, kv_rs, q_ss, q_rs, o_ss, o_rs, y_ss, y_rs, z_ss, z_rs):
    rows, width = x_ref.shape
    half_rows = rows // HALVES
    inner = n * hpd * hd
    gcols = group * hpd * hd
    ngroups = n // group
    stages = width // gcols
    ff_half = wg_ref.shape[1] // 2
    nup = ff_half // chunk
    ndown = width // chunk
    nsteps = nup + ndown
    me = lax.axis_index('seq')
    core = lax.rem(me, 2)
    partner = me + 1 - 2 * core
    mygrp = me // group

    order = sorted(range(ngroups), key=lambda d: -min(d, ngroups - d))

    def grp_of(g):
        off = 0
        for i, d in enumerate(order):
            off = jnp.where(g == i, d, off)
        return lax.rem(mygrp + off, ngroups)

    def tile_copy(s, t, g):
        col = pl.multiple_of(t * inner + grp_of(g) * gcols, 128)
        slot = pl.multiple_of(lax.rem(s, stages) * gcols, 128)
        return pltpu.make_async_copy(wqkv_ref.at[:, pl.ds(col, gcols)], wout.at[:, pl.ds(slot, gcols)],
                                     stage_sem.at[lax.rem(s, stages)])

    def start_tile(s):
        @pl.when(s < 2 * ngroups)
        def _():
            tile_copy(s, 1 + lax.rem(s, 2), s // 2).start()

        @pl.when(jnp.logical_and(s >= 2 * ngroups, s < 3 * ngroups))
        def _():
            tile_copy(s, 0, s - 2 * ngroups).start()

    def up_copies(c, slot):
        ff = pl.multiple_of(core * ff_half + c * chunk, 128)
        return (pltpu.make_async_copy(wg_ref.at[:, pl.ds(ff, chunk)], wbuf.at[slot, 0:width], w_sem.at[slot, 0]),
                pltpu.make_async_copy(wu_ref.at[:, pl.ds(ff, chunk)], wbuf.at[slot, width:2 * width], w_sem.at[slot, 1]))

    def down_copies(c, slot):
        col = pl.multiple_of(c * chunk, 128)
        return tuple(pltpu.make_async_copy(wd_ref.at[pl.ds(core * ff_half + p * width, width), pl.ds(col, chunk)],
                                           wbuf.at[slot, p * width:(p + 1) * width], w_sem.at[slot, p]) for p in range(2))

    def start_up(c):
        for copy in up_copies(c, lax.rem(c, slots)):
            copy.start()

    def down_slot(c):
        return slots - 1 - c % slots

    def start_down(c):
        for copy in down_copies(c, down_slot(c)):
            copy.start()

    inputs = [pltpu.make_async_copy(src, dst, in_sem.at[i]) for i, (src, dst) in enumerate(
        [(xin_ref, x_ref), (gain_refs, ga_ref), (cosin_ref, cos_ref), (sinin_ref, sin_ref), (gainm_refs, gm_ref)])]
    inputs[0].start()
    inputs[1].start()
    for s in range(stages):
        start_tile(s)
    for copy in inputs[2:]:
        copy.start()

    barrier = pltpu.get_barrier_semaphore()

    def greet(k, c):
        pl.semaphore_signal(barrier, inc=1, device_id={'seq': lax.rem(me + k, n)}, device_id_type=MESH)
        return c

    lax.fori_loop(1, n, greet, 0)
    def gain(ref):
        return jnp.concatenate([ref[r:r + 1, :] for r in range(ref.shape[0])], axis=1)

    inputs[0].wait()
    inputs[1].wait()
    yn[1] = rms_norm(x_ref[...], gain(ga_ref)).reshape(2, half_rows, width)

    def remote(src, dst, ssem, rsem, dest):
        return pltpu.make_async_remote_copy(src_ref=src, dst_ref=dst, send_sem=ssem, recv_sem=rsem,
                                            device_id={'seq': dest}, device_id_type=MESH)

    def kv_part(ref, u):
        return ref.at[1] if u == 2 else ref.at[0, u * hd:(u + 1) * hd]

    def kv_send(dest, u):
        return remote(kv_part(kvs.at[dest], u), kv_part(kvr.at[me], u), kv_ss.at[dest, u], kv_rs.at[me, u], dest)

    def kv_recv(src, u):
        return remote(kv_part(kvs.at[src], u), kv_part(kvr.at[src], u), kv_ss.at[src, u], kv_rs.at[src, u], src)

    def kv_local(u):
        return pltpu.make_async_copy(kv_part(kvs.at[me], u), kv_part(kvr.at[me], u), kv_rs.at[me, u])

    def q_send(dest, u):
        src, dst = (qs.at[dest, 0], qr.at[me, 0]) if u == 0 else (qs.at[dest, 1, u - 1], qr.at[me, 1, u - 1])
        return remote(src, dst, q_ss.at[dest, u], q_rs.at[me, u], dest)

    def q_recv(src, u):
        a, b = (qs.at[src, 0], qr.at[src, 0]) if u == 0 else (qs.at[src, 1, u - 1], qr.at[src, 1, u - 1])
        return remote(a, b, q_ss.at[src, u], q_rs.at[src, u], src)

    def q_local(u):
        src, dst = (qs.at[me, 0], qr.at[me, 0]) if u == 0 else (qs.at[me, 1, u - 1], qr.at[me, 1, u - 1])
        return pltpu.make_async_copy(src, dst, q_rs.at[me, u])

    def o_send(dest, f):
        return remote(osend.at[f, dest], orecv.at[f, me], o_ss.at[f, dest], o_rs.at[f, me], dest)

    def o_recv(src, f):
        return remote(osend.at[f, src], orecv.at[f, src], o_ss.at[f, src], o_rs.at[f, src], src)

    def o_local(f):
        return pltpu.make_async_copy(osend.at[f, me], orecv.at[f, me], o_rs.at[f, me])

    def project(s):
        start = pl.multiple_of(lax.rem(s, stages) * gcols, 128)
        out = jnp.dot(yn[1].reshape(rows, width), wout[:, pl.ds(start, gcols)], preferred_element_type=jnp.float32)
        start_tile(s + stages)
        return out.T

    def rope(u):
        lo, hi = u[:hd // 2], u[hd // 2:]
        cos, sin = cos_ref[...], sin_ref[...]
        return jnp.concatenate([lo * cos - hi * sin, hi * cos + lo * sin], axis=0)

    def send_group(g, make):
        def one(k, c):
            dest = grp_of(g) * group + k

            @pl.when(dest != me)
            def _():
                make(dest).start()
            return c

        lax.fori_loop(0, group, one, 0)

    def project_kv(g, c):
        for t in (0, 1):
            tile_copy(2 * g + t, 1 + t, g).wait()
            out = project(2 * g + t)
            if t == 0:
                @pl.when(g == 0)
                def _():
                    inputs[2].wait()
                    inputs[3].wait()
            for k in range(group * hpd):
                u = out[k * hd:(k + 1) * hd]
                if t == 0:
                    u = rope(u)
                kvs[grp_of(g) * group + k // hpd, k % hpd, t * hd:(t + 1) * hd, :] = u.astype(jnp.bfloat16)
            if t == 0:
                @pl.when(g == 0)
                def _():
                    pl.semaphore_wait(barrier, n - 1)

            send_group(g, lambda dest: kv_send(dest, t))
        return c

    lax.fori_loop(0, ngroups, project_kv, 0)
    for u in range(3):
        kv_local(u).start()

    def project_q(g, c):
        s = 2 * ngroups + g
        tile_copy(s, 0, g).wait()
        out = project(s)
        for k in range(group * hpd):
            u = rope(out[k * hd:(k + 1) * hd]).astype(jnp.bfloat16)
            for f in range(HALVES):
                qs[grp_of(g) * group + k // hpd, k % hpd, f] = u[:, f * half_rows:(f + 1) * half_rows]
        send_group(g, lambda dest: q_send(dest, 0))
        return c

    lax.fori_loop(0, ngroups, project_q, 0)
    for u in range(3):
        q_local(u).start()

    def to_others(make):
        def one(k, c):
            make(lax.rem(me + k, n)).start()
            return c

        lax.fori_loop(1, n, one, 0)

    to_others(lambda dest: kv_send(dest, 2))

    wout_copy = pltpu.make_async_copy(wout_ref, wout, wout_sem)
    wout_copy.start()
    for c in range(slots):
        start_up(c)

    per = 4
    kv_per = 2
    q_tile = per * half_rows
    kv_tile = kv_per * rows
    scale2 = LOG2E * hd ** -0.5

    def arrive_kv(h):
        def one(src, c):
            for u in ((0, 1) if h == 0 else (2,)):
                @pl.when(src != me)
                def _():
                    kv_recv(src, u).wait_recv()

                @pl.when(src == me)
                def _():
                    kv_local(u).wait()

            kbuf[pl.ds(pl.multiple_of(src * rows, rows), rows), :] = kvr[src, h, 0:hd, :].T
            return c

        lax.fori_loop(0, n, one, 0)

    def arrive_q(u):
        def one(k, c):
            q_recv(lax.rem(me + k, n), u).wait_recv()
            return c

        lax.fori_loop(1, n, one, 0)
        q_local(u).wait()

    def attend(h, f):
        def one_tile(i, c):
            q_t = jnp.concatenate([qr[per * i + r, h, f] for r in range(per)], axis=1)

            def scores(j, q, blocks=kv_per):
                size = blocks * rows
                k_blk = kbuf[pl.ds(pl.multiple_of(j * size, size), size), :]
                return jnp.dot(k_blk, q, preferred_element_type=jnp.float32)

            def values(j, blocks):
                return jnp.concatenate([kvr[blocks * j + r, h, hd:2 * hd, :] for r in range(blocks)], axis=1)

            def update(j, s, carry, blocks=kv_per):
                m_new = jnp.max(s, axis=0, keepdims=True)
                if carry is not None:
                    m, l, o = carry
                    m_new = jnp.maximum(m, m_new)
                p = jnp.exp2((s - m_new) * scale2)
                l_new = jnp.sum(p, axis=0, keepdims=True)
                o_new = jnp.dot(values(j, blocks), p.astype(jnp.bfloat16), preferred_element_type=jnp.float32)
                if carry is not None:
                    alpha = jnp.exp2((m - m_new) * scale2)
                    l_new = alpha * l + l_new
                    o_new = alpha * o + o_new
                return m_new, l_new, o_new

            def masked(s, off, lane0):
                lane = lane0 + lax.broadcasted_iota(jnp.int32, s.shape, 1)
                query_pos = (lane // half_rows) * rows + f * half_rows + lane % half_rows
                key_pos = off + lax.broadcasted_iota(jnp.int32, s.shape, 0)
                return jnp.where(key_pos <= query_pos, s, -jnp.inf)

            diag = per // kv_per
            cut = q_tile // diag
            first = scores(diag * i, q_t)
            sbuf[1, :, cut:] = scores(diag * i + 1, q_t[:, cut:])
            sbuf[0] = scores(0, q_t)
            carry = update(diag * i, masked(first, 0, 0), None)
            late = update(diag * i + 1, masked(sbuf[1, :, cut:], kv_tile, cut), tuple(v[:, cut:] for v in carry))
            carry = tuple(jnp.concatenate([v[:, :cut], w], axis=1) for v, w in zip(carry, late))
            def pair(t, carry):
                for side in range(2):
                    j = 2 * t + side
                    sbuf[1 - side] = scores(j + 1, q_t)
                    carry = update(j, sbuf[side], carry)
                return carry

            m, l, o = lax.fori_loop(0, diag * i // 2, pair, carry)
            out = (o / l).astype(jnp.bfloat16)
            for r in range(per):
                dest = per * i + r
                osend[f, dest, h] = out[:, r * half_rows:(r + 1) * half_rows]
                if h == hpd - 1:
                    @pl.when(dest != me)
                    def _():
                        o_send(dest, f).start()

                    @pl.when(dest == me)
                    def _():
                        o_local(f).start()
            return c

        lax.fori_loop(0, n // per, one_tile, 0)

    arrive_q(0)
    to_others(lambda dest: q_send(dest, 1))
    to_others(lambda dest: q_send(dest, 2))
    arrive_kv(0)
    attend(0, 0)
    attend(0, 1)
    arrive_kv(1)
    arrive_q(1)
    attend(1, 0)
    arrive_q(2)
    attend(1, 1)
    wout_copy.wait()
    inputs[4].wait()

    def y_send(f):
        return remote(yn.at[f, 0], yn.at[f, 1], y_ss.at[f], y_rs.at[f], partner)

    def z_send(c):
        return remote(zsend.at[c], zrecv.at[c], z_ss.at[c], z_rs.at[c], partner)

    def out_projection(f):
        r0 = f * half_rows

        def arrive_o(k, c):
            o_recv(lax.rem(me + k, n), f).wait_recv()
            return c

        lax.fori_loop(1, n, arrive_o, 0)
        o_local(f).wait()
        o_rows = orecv[f].reshape(inner, half_rows).T
        mixed = jnp.dot(o_rows, wout[...], preferred_element_type=jnp.float32)
        y = (x_ref[r0:r0 + half_rows, :].astype(jnp.float32) + mixed).astype(jnp.bfloat16)
        x_ref[r0:r0 + half_rows, :] = y
        yn[f, 0] = rms_norm(y, gain(gm_ref))
        y_send(f).start()

    def gate_up(f, first, last):
        def one(t, carry):
            c = t if f == 0 else nup - 1 - t
            slot = lax.rem(c, slots)
            if f == 0:
                for copy in up_copies(c, slot):
                    copy.wait()
            else:
                @pl.when(t >= slots)
                def _():
                    for copy in up_copies(c, slot):
                        copy.wait()
            y_all = yn[f].reshape(2 * half_rows, width)
            gate = jnp.dot(y_all, wbuf[slot, 0:width], preferred_element_type=jnp.float32)
            up = jnp.dot(y_all, wbuf[slot, width:2 * width], preferred_element_type=jnp.float32)
            cols = pl.ds(pl.multiple_of(c * chunk, 128), chunk)
            hidden[f, :, cols] = (gate / (1.0 + jnp.exp(-gate)) * up).astype(jnp.bfloat16)
            if f == 0:
                @pl.when(c + slots < nup)
                def _():
                    start_up(c + slots)
            else:
                @pl.when(c >= slots)
                def _():
                    start_up(c - slots)

                @pl.when(c < slots)
                def _():
                    start_down(slots - 1 - c)
            return carry

        lax.fori_loop(first, last, one, 0)

    def down(first, last):
        def one(c, carry):
            slot = down_slot(c)
            for copy in down_copies(c, slot):
                copy.wait()
            part = jnp.dot(hidden[...].reshape(HALVES * rows, ff_half), wbuf[slot], preferred_element_type=jnp.float32)
            part = part.reshape(HALVES, 2, half_rows, chunk)
            zsend[c] = part[:, 1]
            z_send(c).start()
            zown[c] = part[:, 0]

            @pl.when(c + slots < ndown)
            def _():
                start_down(c + slots)
            return carry

        lax.fori_loop(first, last, one, 0)

    def finish(c):
        z_send(c).wait()
        cols = slice(c * chunk, (c + 1) * chunk)
        total = (zown[c] + zrecv[c]).reshape(rows, chunk)
        z_ref[:, cols] = (x_ref[:, cols].astype(jnp.float32) + total).astype(jnp.bfloat16)

    def early(r):
        for c in range(2):
            if r == 0:
                for copy in up_copies(c, c):
                    copy.wait()
            gate = jnp.dot(yn[0, r], wbuf[c, 0:width], preferred_element_type=jnp.float32)
            up = jnp.dot(yn[0, r], wbuf[c, width:2 * width], preferred_element_type=jnp.float32)
            silu = gate / (1.0 + jnp.exp(-gate))
            hidden[0, r * half_rows:(r + 1) * half_rows, c * chunk:(c + 1) * chunk] = (silu * up).astype(jnp.bfloat16)
            if r == 1:
                start_up(c + slots)

    out_projection(0)
    early(0)
    y_send(0).wait()
    early(1)
    gate_up(0, 2, nup - 2)
    out_projection(1)
    gate_up(0, nup - 2, nup)
    y_send(1).wait()
    gate_up(1, 0, nup)
    down(0, ndown - 1)
    for c in range(ndown - 2):
        finish(c)
    last = ndown - 1
    for copy in down_copies(last, down_slot(last)):
        copy.wait()
    for r, dst in ((1, zsend), (0, zown)):
        rows_in = hidden[:, r * half_rows:(r + 1) * half_rows, :].reshape(HALVES * half_rows, ff_half)
        part = jnp.dot(rows_in, wbuf[down_slot(last)], preferred_element_type=jnp.float32)
        dst[last] = part.reshape(HALVES, half_rows, chunk)
        if r == 1:
            z_send(last).start()
    for c in range(ndown - 2, ndown):
        finish(c)

    def drain(k, c):
        other = lax.rem(me + k, n)
        for u in range(3):
            kv_send(other, u).wait_send()
            q_send(other, u).wait_send()
        for f in range(HALVES):
            o_send(other, f).wait_send()
        return c

    lax.fori_loop(1, n, drain, 0)


def solution(mesh):
    n = mesh.shape['seq']

    def local_layer(x_blk, g_attn, w_qkv, w_out, g_mlp, w_gate, w_up, w_down):
        n_heads, hd, width = w_out.shape
        rows = x_blk.shape[0]
        hpd = n_heads // n
        member = lax.axis_index('seq')
        cos_t, sin_t = rope_tables_t(member * rows + jnp.arange(rows), hd)
        group = 1
        while (group * hpd * hd) % 128:
            group *= 2
        chunk, slots = 512, 3
        half = rows // HALVES
        bf16, f32 = jnp.bfloat16, jnp.float32
        vmem = pl.BlockSpec(memory_space=pltpu.VMEM)
        hbm = pl.BlockSpec(memory_space=pl.ANY)
        dma = pltpu.SemaphoreType.DMA
        return pl.pallas_call(
            functools.partial(layer_kernel, n, hpd, hd, group, chunk, slots),
            out_shape=pltpu.VMEM(x_blk.shape, bf16),
            in_specs=[hbm] * 10,
            out_specs=vmem,
            scratch_shapes=[
                pltpu.VMEM((rows, width), bf16),
                pltpu.VMEM((width // 128, 128), f32),
                pltpu.VMEM((width // 128, 128), f32),
                pltpu.VMEM((hd // 2, rows), f32),
                pltpu.VMEM((hd // 2, rows), f32),
                pltpu.VMEM((n_heads * hd, width), bf16),
                pltpu.VMEM((n, hpd, 2 * hd, rows), bf16),
                pltpu.VMEM((n, hpd, 2 * hd, rows), bf16),
                pltpu.VMEM((n, hpd, HALVES, hd, half), bf16),
                pltpu.VMEM((n, hpd, HALVES, hd, half), bf16),
                pltpu.VMEM((n * rows, hd), bf16),
                pltpu.VMEM((2, 2 * rows, 4 * half), f32),
                pltpu.VMEM((HALVES, n, hpd, hd, half), bf16),
                pltpu.VMEM((HALVES, n, hpd, hd, half), bf16),
                pltpu.VMEM((HALVES, 2, half, width), bf16),
                pltpu.VMEM((HALVES, rows, w_down.shape[0] // 2), bf16),
                pltpu.VMEM((width // chunk, HALVES, half, chunk), f32),
                pltpu.VMEM((width // chunk, HALVES, half, chunk), f32),
                pltpu.VMEM((width // chunk, HALVES, half, chunk), f32),
                pltpu.VMEM((slots, 2 * width, chunk), bf16),
                dma((5,)), dma((4,)), dma, dma((slots, 2)),
                dma((n, 3)), dma((n, 3)), dma((n, 3)), dma((n, 3)), dma((HALVES, n)), dma((HALVES, n)),
                dma((HALVES,)), dma((HALVES,)), dma((width // chunk,)), dma((width // chunk,)),
            ],
            compiler_params=pltpu.CompilerParams(collective_id=0, has_side_effects=True, vmem_limit_bytes=64 * 1000 * 1024),
            name='layer',
        )(x_blk, g_attn.reshape(-1, 128), g_mlp.reshape(-1, 128), cos_t, sin_t, w_qkv, w_out.reshape(n_heads * hd, width), w_gate, w_up, w_down)

    row_spec = P(('data', 'seq'), None)
    return jax.shard_map(local_layer, mesh=mesh, in_specs=(row_spec, P(), P(), P(), P(), P(), P(), P()), out_specs=row_spec, check_vma=False)
```

```python
import functools
import math

import jax
import jax.numpy as jnp
import numpy as np
from jax import lax
from jax.experimental import pallas as pl
from jax.experimental.pallas import tpu as pltpu
from jax.sharding import PartitionSpec as P

ROPE_BASE = 10000
LOG2E = math.log2(math.e)
HALVES = 2
MESH = pl.DeviceIdType.MESH


def rms_norm(row_vals, gain_vec):
    rows_f32 = row_vals.astype(jnp.float32)
    inv_rms = lax.rsqrt(jnp.mean(rows_f32 * rows_f32, axis=-1, keepdims=True) + 1e-5)
    return (rows_f32 * inv_rms * gain_vec).astype(jnp.bfloat16)


def rope_parts(n, rows, head_dim):
    freq = 1.0 / (float(ROPE_BASE) ** (np.arange(0, head_dim, 2, dtype=np.float64) / head_dim))
    local = freq[:, None] * np.arange(rows)
    start = np.zeros((head_dim // 2, 128))
    start[:, :n] = freq[:, None] * (np.arange(n) * rows)
    return tuple(np.stack([np.cos(v), np.sin(v)]).astype(np.float32) for v in (local, start))


def layer_kernel(n, hpd, hd, group, chunk, slots,
                 xin_ref, gain_refs, gainm_refs, angle_ref, start_ref, wqkv_ref, wout_ref, wg_ref, wu_ref, wd_ref, z_ref,
                 x_ref, ga_ref, gm_ref, angle, angle0, cos_ref, sin_ref, wout, kvs, kvr, qs, qr, kbuf, sbuf, osend, orecv, yn, hidden, zown, zsend, zrecv, wbuf,
                 in_sem, stage_sem, wout_sem, w_sem, kv_ss, kv_rs, q_ss, q_rs, o_ss, o_rs, y_ss, y_rs, z_ss, z_rs):
    rows, width = x_ref.shape
    half_rows = rows // HALVES
    inner = n * hpd * hd
    gcols = group * hpd * hd
    ngroups = n // group
    stages = width // gcols
    ff_half = wg_ref.shape[1] // 2
    nup = ff_half // chunk
    ndown = width // chunk
    nsteps = nup + ndown
    me = lax.axis_index('seq')
    core = lax.rem(me, 2)
    partner = me + 1 - 2 * core
    mygrp = me // group

    order = sorted(range(ngroups), key=lambda d: -min(d, ngroups - d))

    def grp_of(g):
        off = 0
        for i, d in enumerate(order):
            off = jnp.where(g == i, d, off)
        return lax.rem(mygrp + off, ngroups)

    def tile_copy(s, t, g):
        col = pl.multiple_of(t * inner + grp_of(g) * gcols, 128)
        slot = pl.multiple_of(lax.rem(s, stages) * gcols, 128)
        return pltpu.make_async_copy(wqkv_ref.at[:, pl.ds(col, gcols)], wout.at[:, pl.ds(slot, gcols)],
                                     stage_sem.at[lax.rem(s, stages)])

    def start_tile(s):
        @pl.when(s < 2 * ngroups)
        def _():
            tile_copy(s, 1 + lax.rem(s, 2), s // 2).start()

        @pl.when(jnp.logical_and(s >= 2 * ngroups, s < 3 * ngroups))
        def _():
            tile_copy(s, 0, s - 2 * ngroups).start()

    def up_copies(c, slot):
        ff = pl.multiple_of(core * ff_half + c * chunk, 128)
        return (pltpu.make_async_copy(wg_ref.at[:, pl.ds(ff, chunk)], wbuf.at[slot, 0:width], w_sem.at[slot, 0]),
                pltpu.make_async_copy(wu_ref.at[:, pl.ds(ff, chunk)], wbuf.at[slot, width:2 * width], w_sem.at[slot, 1]))

    def down_copies(c, slot):
        col = pl.multiple_of(c * chunk, 128)
        return tuple(pltpu.make_async_copy(wd_ref.at[pl.ds(core * ff_half + p * width, width), pl.ds(col, chunk)],
                                           wbuf.at[slot, p * width:(p + 1) * width], w_sem.at[slot, p]) for p in range(2))

    def start_up(c):
        for copy in up_copies(c, lax.rem(c, slots)):
            copy.start()

    def down_slot(c):
        return slots - 1 - c % slots

    def start_down(c):
        for copy in down_copies(c, down_slot(c)):
            copy.start()

    inputs = [pltpu.make_async_copy(src, dst, in_sem.at[i]) for i, (src, dst) in enumerate(
        [(xin_ref, x_ref), (gain_refs, ga_ref), (angle_ref, angle), (start_ref, angle0), (gainm_refs, gm_ref)])]
    inputs[0].start()
    inputs[1].start()
    for s in range(stages):
        start_tile(s)
    for copy in inputs[2:]:
        copy.start()

    barrier = pltpu.get_barrier_semaphore()

    def greet(k, c):
        pl.semaphore_signal(barrier, inc=1, device_id={'seq': lax.rem(me + k, n)}, device_id_type=MESH)
        return c

    lax.fori_loop(1, n, greet, 0)
    def gain(ref):
        return jnp.concatenate([ref[r:r + 1, :] for r in range(ref.shape[0])], axis=1)

    inputs[0].wait()
    inputs[1].wait()
    yn[1] = rms_norm(x_ref[...], gain(ga_ref)).reshape(2, half_rows, width)

    def remote(src, dst, ssem, rsem, dest):
        return pltpu.make_async_remote_copy(src_ref=src, dst_ref=dst, send_sem=ssem, recv_sem=rsem,
                                            device_id={'seq': dest}, device_id_type=MESH)

    def kv_part(ref, u):
        return ref.at[1] if u == 2 else ref.at[0, u * hd:(u + 1) * hd]

    def kv_send(dest, u):
        return remote(kv_part(kvs.at[dest], u), kv_part(kvr.at[me], u), kv_ss.at[dest, u], kv_rs.at[me, u], dest)

    def kv_recv(src, u):
        return remote(kv_part(kvs.at[src], u), kv_part(kvr.at[src], u), kv_ss.at[src, u], kv_rs.at[src, u], src)

    def kv_local(u):
        return pltpu.make_async_copy(kv_part(kvs.at[me], u), kv_part(kvr.at[me], u), kv_rs.at[me, u])

    def q_send(dest, u):
        src, dst = (qs.at[dest, 0], qr.at[me, 0]) if u == 0 else (qs.at[dest, 1, u - 1], qr.at[me, 1, u - 1])
        return remote(src, dst, q_ss.at[dest, u], q_rs.at[me, u], dest)

    def q_recv(src, u):
        a, b = (qs.at[src, 0], qr.at[src, 0]) if u == 0 else (qs.at[src, 1, u - 1], qr.at[src, 1, u - 1])
        return remote(a, b, q_ss.at[src, u], q_rs.at[src, u], src)

    def q_local(u):
        src, dst = (qs.at[me, 0], qr.at[me, 0]) if u == 0 else (qs.at[me, 1, u - 1], qr.at[me, 1, u - 1])
        return pltpu.make_async_copy(src, dst, q_rs.at[me, u])

    def o_send(dest, f):
        return remote(osend.at[f, dest], orecv.at[f, me], o_ss.at[f, dest], o_rs.at[f, me], dest)

    def o_recv(src, f):
        return remote(osend.at[f, src], orecv.at[f, src], o_ss.at[f, src], o_rs.at[f, src], src)

    def o_local(f):
        return pltpu.make_async_copy(osend.at[f, me], orecv.at[f, me], o_rs.at[f, me])

    def project(s):
        start = pl.multiple_of(lax.rem(s, stages) * gcols, 128)
        out = jnp.dot(yn[1].reshape(rows, width), wout[:, pl.ds(start, gcols)], preferred_element_type=jnp.float32)
        start_tile(s + stages)
        return out.T

    def rope(u):
        lo, hi = u[:hd // 2], u[hd // 2:]
        cos, sin = cos_ref[...], sin_ref[...]
        return jnp.concatenate([lo * cos - hi * sin, hi * cos + lo * sin], axis=0)

    def send_group(g, make):
        def one(k, c):
            dest = grp_of(g) * group + k

            @pl.when(dest != me)
            def _():
                make(dest).start()
            return c

        lax.fori_loop(0, group, one, 0)

    def project_kv(g, c):
        for t in (0, 1):
            tile_copy(2 * g + t, 1 + t, g).wait()
            out = project(2 * g + t)
            if t == 0:
                @pl.when(g == 0)
                def _():
                    inputs[2].wait()
                    inputs[3].wait()
                    mine = lax.broadcasted_iota(jnp.int32, angle0.shape, 2) == me
                    c0, s0 = jnp.sum(jnp.where(mine, angle0[...], 0.0), axis=2, keepdims=True)
                    cos_ref[...] = angle[0] * c0 - angle[1] * s0
                    sin_ref[...] = angle[1] * c0 + angle[0] * s0
            for k in range(group * hpd):
                u = out[k * hd:(k + 1) * hd]
                if t == 0:
                    u = rope(u)
                kvs[grp_of(g) * group + k // hpd, k % hpd, t * hd:(t + 1) * hd, :] = u.astype(jnp.bfloat16)
            if t == 0:
                @pl.when(g == 0)
                def _():
                    pl.semaphore_wait(barrier, n - 1)

            send_group(g, lambda dest: kv_send(dest, t))
        return c

    lax.fori_loop(0, ngroups, project_kv, 0)
    for u in range(3):
        kv_local(u).start()

    def project_q(g, c):
        s = 2 * ngroups + g
        tile_copy(s, 0, g).wait()
        out = project(s)
        for k in range(group * hpd):
            u = rope(out[k * hd:(k + 1) * hd]).astype(jnp.bfloat16)
            for f in range(HALVES):
                qs[grp_of(g) * group + k // hpd, k % hpd, f] = u[:, f * half_rows:(f + 1) * half_rows]
        send_group(g, lambda dest: q_send(dest, 0))
        return c

    lax.fori_loop(0, ngroups, project_q, 0)
    for u in range(3):
        q_local(u).start()

    def to_others(make):
        def one(k, c):
            make(lax.rem(me + k, n)).start()
            return c

        lax.fori_loop(1, n, one, 0)

    to_others(lambda dest: kv_send(dest, 2))

    wout_copy = pltpu.make_async_copy(wout_ref, wout, wout_sem)
    wout_copy.start()
    for c in range(slots):
        start_up(c)

    per = 4
    kv_per = 2
    q_tile = per * half_rows
    kv_tile = kv_per * rows
    scale2 = LOG2E * hd ** -0.5

    def arrive_kv(h):
        def one(src, c):
            for u in ((0, 1) if h == 0 else (2,)):
                @pl.when(src != me)
                def _():
                    kv_recv(src, u).wait_recv()

                @pl.when(src == me)
                def _():
                    kv_local(u).wait()

            kbuf[pl.ds(pl.multiple_of(src * rows, rows), rows), :] = kvr[src, h, 0:hd, :].T
            return c

        lax.fori_loop(0, n, one, 0)

    def arrive_q(u):
        def one(k, c):
            q_recv(lax.rem(me + k, n), u).wait_recv()
            return c

        lax.fori_loop(1, n, one, 0)
        q_local(u).wait()

    def attend(h, f):
        def one_tile(i, c):
            q_t = jnp.concatenate([qr[per * i + r, h, f] for r in range(per)], axis=1)

            def scores(j, q, blocks=kv_per):
                size = blocks * rows
                k_blk = kbuf[pl.ds(pl.multiple_of(j * size, size), size), :]
                return jnp.dot(k_blk, q, preferred_element_type=jnp.float32)

            def values(j, blocks):
                return jnp.concatenate([kvr[blocks * j + r, h, hd:2 * hd, :] for r in range(blocks)], axis=1)

            def update(j, s, carry, blocks=kv_per):
                m_new = jnp.max(s, axis=0, keepdims=True)
                if carry is not None:
                    m, l, o = carry
                    m_new = jnp.maximum(m, m_new)
                p = jnp.exp2((s - m_new) * scale2)
                l_new = jnp.sum(p, axis=0, keepdims=True)
                o_new = jnp.dot(values(j, blocks), p.astype(jnp.bfloat16), preferred_element_type=jnp.float32)
                if carry is not None:
                    alpha = jnp.exp2((m - m_new) * scale2)
                    l_new = alpha * l + l_new
                    o_new = alpha * o + o_new
                return m_new, l_new, o_new

            def masked(s, off, lane0):
                lane = lane0 + lax.broadcasted_iota(jnp.int32, s.shape, 1)
                query_pos = (lane // half_rows) * rows + f * half_rows + lane % half_rows
                key_pos = off + lax.broadcasted_iota(jnp.int32, s.shape, 0)
                return jnp.where(key_pos <= query_pos, s, -jnp.inf)

            diag = per // kv_per
            cut = q_tile // diag
            first = scores(diag * i, q_t)
            sbuf[1, :, cut:] = scores(diag * i + 1, q_t[:, cut:])
            sbuf[0] = scores(0, q_t)
            carry = update(diag * i, masked(first, 0, 0), None)
            late = update(diag * i + 1, masked(sbuf[1, :, cut:], kv_tile, cut), tuple(v[:, cut:] for v in carry))
            carry = tuple(jnp.concatenate([v[:, :cut], w], axis=1) for v, w in zip(carry, late))
            def pair(t, carry):
                for side in range(2):
                    j = 2 * t + side
                    sbuf[1 - side] = scores(j + 1, q_t)
                    carry = update(j, sbuf[side], carry)
                return carry

            m, l, o = lax.fori_loop(0, diag * i // 2, pair, carry)
            out = (o / l).astype(jnp.bfloat16)
            for r in range(per):
                dest = per * i + r
                osend[f, dest, h] = out[:, r * half_rows:(r + 1) * half_rows]
            return c

        lax.fori_loop(0, n // per, one_tile, 0)
        if h == hpd - 1:
            to_others(lambda dest: o_send(dest, f))
            o_local(f).start()

    arrive_q(0)
    to_others(lambda dest: q_send(dest, 1))
    to_others(lambda dest: q_send(dest, 2))
    arrive_kv(0)
    attend(0, 0)
    attend(0, 1)
    arrive_kv(1)
    arrive_q(1)
    attend(1, 0)
    arrive_q(2)
    attend(1, 1)
    wout_copy.wait()
    inputs[4].wait()

    def y_send(f):
        return remote(yn.at[f, 0], yn.at[f, 1], y_ss.at[f], y_rs.at[f], partner)

    def z_send(c):
        return remote(zsend.at[c], zrecv.at[c], z_ss.at[c], z_rs.at[c], partner)

    def out_projection(f):
        r0 = f * half_rows

        def arrive_o(k, c):
            o_recv(lax.rem(me + k, n), f).wait_recv()
            return c

        lax.fori_loop(1, n, arrive_o, 0)
        o_local(f).wait()
        o_rows = orecv[f].reshape(inner, half_rows).T
        mixed = jnp.dot(o_rows, wout[...], preferred_element_type=jnp.float32)
        y = (x_ref[r0:r0 + half_rows, :].astype(jnp.float32) + mixed).astype(jnp.bfloat16)
        x_ref[r0:r0 + half_rows, :] = y
        yn[f, 0] = rms_norm(y, gain(gm_ref))
        y_send(f).start()

    def gate_up(f, first, last):
        def one(t, carry):
            c = t if f == 0 else nup - 1 - t
            slot = lax.rem(c, slots)
            if f == 0:
                for copy in up_copies(c, slot):
                    copy.wait()
            else:
                @pl.when(t >= slots)
                def _():
                    for copy in up_copies(c, slot):
                        copy.wait()
            y_all = yn[f].reshape(2 * half_rows, width)
            gate = jnp.dot(y_all, wbuf[slot, 0:width], preferred_element_type=jnp.float32)
            up = jnp.dot(y_all, wbuf[slot, width:2 * width], preferred_element_type=jnp.float32)
            cols = pl.ds(pl.multiple_of(c * chunk, 128), chunk)
            hidden[f, :, cols] = (gate / (1.0 + jnp.exp(-gate)) * up).astype(jnp.bfloat16)
            if f == 0:
                @pl.when(c + slots < nup)
                def _():
                    start_up(c + slots)
            else:
                @pl.when(c >= slots)
                def _():
                    start_up(c - slots)

                @pl.when(c < slots)
                def _():
                    start_down(slots - 1 - c)
            return carry

        lax.fori_loop(first, last, one, 0)

    def down(first, last):
        def one(c, carry):
            slot = down_slot(c)
            for copy in down_copies(c, slot):
                copy.wait()
            part = jnp.dot(hidden[...].reshape(HALVES * rows, ff_half), wbuf[slot], preferred_element_type=jnp.float32)
            part = part.reshape(HALVES, 2, half_rows, chunk)
            zsend[c] = part[:, 1]
            z_send(c).start()
            zown[c] = part[:, 0]

            @pl.when(c + slots < ndown)
            def _():
                start_down(c + slots)
            return carry

        lax.fori_loop(first, last, one, 0)

    def finish(c):
        z_send(c).wait()
        cols = slice(c * chunk, (c + 1) * chunk)
        total = (zown[c] + zrecv[c]).reshape(rows, chunk)
        z_ref[:, cols] = (x_ref[:, cols].astype(jnp.float32) + total).astype(jnp.bfloat16)

    def early(r):
        for c in range(2):
            if r == 0:
                for copy in up_copies(c, c):
                    copy.wait()
            gate = jnp.dot(yn[0, r], wbuf[c, 0:width], preferred_element_type=jnp.float32)
            up = jnp.dot(yn[0, r], wbuf[c, width:2 * width], preferred_element_type=jnp.float32)
            silu = gate / (1.0 + jnp.exp(-gate))
            hidden[0, r * half_rows:(r + 1) * half_rows, c * chunk:(c + 1) * chunk] = (silu * up).astype(jnp.bfloat16)
            if r == 1:
                start_up(c + slots)

    out_projection(0)
    early(0)
    y_send(0).wait()
    early(1)
    gate_up(0, 2, nup - 2)
    out_projection(1)
    gate_up(0, nup - 2, nup)
    y_send(1).wait()
    gate_up(1, 0, nup)
    down(0, ndown - 1)
    for c in range(ndown - 2):
        finish(c)
    last = ndown - 1
    for copy in down_copies(last, down_slot(last)):
        copy.wait()
    for r, dst in ((1, zsend), (0, zown)):
        rows_in = hidden[:, r * half_rows:(r + 1) * half_rows, :].reshape(HALVES * half_rows, ff_half)
        part = jnp.dot(rows_in, wbuf[down_slot(last)], preferred_element_type=jnp.float32)
        dst[last] = part.reshape(HALVES, half_rows, chunk)
        if r == 1:
            z_send(last).start()
    for c in range(ndown - 2, ndown):
        finish(c)

    def drain(k, c):
        other = lax.rem(me + k, n)
        for u in range(3):
            kv_send(other, u).wait_send()
            q_send(other, u).wait_send()
        for f in range(HALVES):
            o_send(other, f).wait_send()
        return c

    lax.fori_loop(1, n, drain, 0)


def solution(mesh):
    n = mesh.shape['seq']

    def local_layer(x_blk, g_attn, w_qkv, w_out, g_mlp, w_gate, w_up, w_down):
        n_heads, hd, width = w_out.shape
        rows = x_blk.shape[0]
        hpd = n_heads // n
        angles, starts = (jnp.asarray(v) for v in rope_parts(n, rows, hd))
        group = 1
        while (group * hpd * hd) % 128:
            group *= 2
        chunk, slots = 512, 3
        half = rows // HALVES
        bf16, f32 = jnp.bfloat16, jnp.float32
        vmem = pl.BlockSpec(memory_space=pltpu.VMEM)
        hbm = pl.BlockSpec(memory_space=pl.ANY)
        dma = pltpu.SemaphoreType.DMA
        return pl.pallas_call(
            functools.partial(layer_kernel, n, hpd, hd, group, chunk, slots),
            out_shape=pltpu.VMEM(x_blk.shape, bf16),
            in_specs=[hbm] * 10,
            out_specs=vmem,
            scratch_shapes=[
                pltpu.VMEM((rows, width), bf16),
                pltpu.VMEM((width // 128, 128), f32),
                pltpu.VMEM((width // 128, 128), f32),
                pltpu.VMEM((2, hd // 2, rows), f32),
                pltpu.VMEM((2, hd // 2, 128), f32),
                pltpu.VMEM((hd // 2, rows), f32),
                pltpu.VMEM((hd // 2, rows), f32),
                pltpu.VMEM((n_heads * hd, width), bf16),
                pltpu.VMEM((n, hpd, 2 * hd, rows), bf16),
                pltpu.VMEM((n, hpd, 2 * hd, rows), bf16),
                pltpu.VMEM((n, hpd, HALVES, hd, half), bf16),
                pltpu.VMEM((n, hpd, HALVES, hd, half), bf16),
                pltpu.VMEM((n * rows, hd), bf16),
                pltpu.VMEM((2, 2 * rows, 4 * half), f32),
                pltpu.VMEM((HALVES, n, hpd, hd, half), bf16),
                pltpu.VMEM((HALVES, n, hpd, hd, half), bf16),
                pltpu.VMEM((HALVES, 2, half, width), bf16),
                pltpu.VMEM((HALVES, rows, w_down.shape[0] // 2), bf16),
                pltpu.VMEM((width // chunk, HALVES, half, chunk), f32),
                pltpu.VMEM((width // chunk, HALVES, half, chunk), f32),
                pltpu.VMEM((width // chunk, HALVES, half, chunk), f32),
                pltpu.VMEM((slots, 2 * width, chunk), bf16),
                dma((5,)), dma((4,)), dma, dma((slots, 2)),
                dma((n, 3)), dma((n, 3)), dma((n, 3)), dma((n, 3)), dma((HALVES, n)), dma((HALVES, n)),
                dma((HALVES,)), dma((HALVES,)), dma((width // chunk,)), dma((width // chunk,)),
            ],
            compiler_params=pltpu.CompilerParams(collective_id=0, has_side_effects=True, vmem_limit_bytes=64 * 1000 * 1024),
            name='layer',
        )(x_blk, g_attn.reshape(-1, 128), g_mlp.reshape(-1, 128), angles, starts, w_qkv, w_out.reshape(n_heads * hd, width), w_gate, w_up, w_down)

    row_spec = P(('data', 'seq'), None)
    return jax.shard_map(local_layer, mesh=mesh, in_specs=(row_spec, P(), P(), P(), P(), P(), P(), P()), out_specs=row_spec, check_vma=False)
```
